32 devices in a mesh: section: 2 (over x), blk: 8 (over z, y), head: 2 (over core).
Axes of the slice: x: 2, y: 2, z: 4, core: 2. Of those that a mesh axis runs over, the one named last changes fastest.
Arguments:
- hidden_in: bfloat16 [4, 64, 1536], P(None, 'blk', 'head'), may hold values from -6 to 6
- w_qkv: bfloat16 [2, 1536, 3, 1536], P('section', 'blk', None, 'head'), may hold values from -0.15625 to 0.15625
- norm_gain: float32 [2, 1536], P('section'), may hold values from 0.5 to 1.5
- qk_gain: float32 [2, 2, 128], P('section'), may hold values from 1 to 2
- text_states: bfloat16 [2, 256, 1536], P('section'), may hold values from -6 to 6
- text_len: int32 [1], replicated, may hold values from 64 to 256
- patch_len: int32 [4], replicated, may hold values from 32 to 64
- stale_flags: int32 [4, 2], replicated, may hold values from 0 to 1, as said below
- stale_kv: bfloat16 [2, 2, 4, 64, 1536], P('section', None, None, 'blk', 'head'), may hold values from -6 to 6
Outputs:
- hidden_out: bfloat16 [2, 4, 64, 1536], P('section', None, 'blk', 'head')
- new_cache: bfloat16 [2, 2, 4, 64, 1536], P('section', None, None, 'blk', 'head')
The draws below stay inside these ranges and needn't reach their ends.
Inputs may be any that keep to these rules, and one draw needn't show every extreme that they name: `stale_flags`: 1 means that the micro-batch uses the previous step's keys and values at that layer, 0 that it uses its fresh ones; every layer has at least one micro-batch flagged 1 and at least one flagged 0.
All inputs are finite; a program needn't handle non-finite values.
Results may differ from the reference program's by a relative error of at most 0.02.
Values may be sent and summed in bfloat16 or wider, within the bound.
A program may use at most 64 MiB of HBM per device.

```python
import math
import jax
import jax.numpy as jnp
from jax import lax

D = 1536
HEADS = 12
HEAD_DIM = 128
TEXT = 256
MICRO = 4
LAYERS = 2
PATCH = 64


def draw_stale_flags(key, part):
    bits_key = jax.random.fold_in(key, 101)
    pick_key = jax.random.fold_in(key, 202)
    random_bits = jax.random.randint(bits_key, (MICRO, LAYERS), 0, 2).astype(jnp.int32)
    chosen = jax.random.randint(pick_key, (1, LAYERS), 0, MICRO).astype(jnp.int32)
    rows = jnp.arange(MICRO, dtype=jnp.int32)[:, None]
    forced_on = rows == chosen
    forced_off = rows == (chosen + 1) % MICRO
    flags = jnp.where(forced_on, 1, jnp.where(forced_off, 0, random_bits))
    return flags.astype(jnp.int32)


def plant(array, own_key, low, high):
    spot = [jax.random.randint(jax.random.fold_in(own_key, axis), (), 0, length) for axis, length in enumerate(array.shape)]
    main_axis = array.shape.index(max(array.shape))
    next_to = spot[:main_axis] + [(spot[main_axis] + 1) % array.shape[main_axis]] + spot[main_axis + 1:]
    return array.at[tuple(spot)].set(low).at[tuple(next_to)].set(high)


def levels(rng, extent, pieces, smallest, top_value):
    def one(dim, parts):
        steps = jax.random.uniform(jax.random.fold_in(jax.random.fold_in(rng, 6), dim), (parts,), jnp.float32, smallest / len(pieces), top_value / len(pieces))
        return jnp.repeat(jnp.exp(steps), extent[dim] // parts).reshape((-1,) + (1,) * (len(extent) - dim - 1))

    loudness = one(*pieces[0])
    for cut in pieces[1:]:
        loudness = loudness * one(*cut)
    return loudness


def gaussian(own_key, dims, scale, reach, split=(), kind=jnp.bfloat16):
    result = jax.random.normal(own_key, dims, jnp.float32) * scale
    if len(split) > 0:
        result = levels(own_key, dims, split, -0.22, 0.18) * result
    return jnp.clip(result, min=-reach, max=reach).astype(kind)


def setup_inputs(seed: int = 0) -> dict:
    splits = jax.random.split(jax.random.key(seed), 10)
    hidden_in = gaussian(splits[0], (MICRO, PATCH, D), 1.0, 6.0, ((1, 8), (2, 2)))
    w_qkv = gaussian(splits[1], (LAYERS, D, 3, HEADS * HEAD_DIM), D ** -0.5, 0.15625, ((0, 2), (1, 8), (3, 2)))
    norm_gain = jnp.clip(1.0 + 0.1 * jax.random.normal(splits[2], (LAYERS, D), jnp.float32), 0.5, 1.5)
    qk_gain = jnp.clip(jnp.exp(math.log(2.0) - 0.6931472 * jax.random.uniform(splits[3], (LAYERS, 2, HEAD_DIM), jnp.float32) ** levels(splits[3], (LAYERS, 2, HEAD_DIM), ((0, 2),), -0.2, 0.2)), 1.0, 2.0)
    text_states = gaussian(splits[4], (LAYERS, TEXT, D), 1.0, 6.0, ((0, 2),))
    text_len = jax.random.randint(splits[5], (1,), TEXT // 4, TEXT + 1).astype(jnp.int32)
    patch_len = plant(jax.random.randint(splits[6], (MICRO,), PATCH // 2, PATCH + 1), jax.random.fold_in(splits[6], 1), PATCH // 2, PATCH).astype(jnp.int32)
    stale_flags = draw_stale_flags(jax.random.fold_in(splits[9], 71), 0)
    stale_kv = gaussian(splits[8], (LAYERS, 2, MICRO, PATCH, HEADS * HEAD_DIM), 1.0, 6.0, ((0, 2), (3, 8), (4, 2)))
    return dict(hidden_in=hidden_in, w_qkv=w_qkv, norm_gain=norm_gain, qk_gain=qk_gain, text_states=text_states, text_len=text_len, patch_len=patch_len, stale_flags=stale_flags, stale_kv=stale_kv)


def norm_rows(values, row_gain):
    return values * lax.rsqrt(lax.optimization_barrier(jnp.mean(values * values, axis=-1, keepdims=True)) + 1e-06) * row_gain

def attend_part(queries, key_rows, value_rows, key_mask):
    scores = jnp.einsum('qhd,khd->hqk', queries.astype(jnp.float32), key_rows.astype(jnp.float32), precision=lax.Precision.HIGHEST) * HEAD_DIM ** (-0.5)
    probs = jnp.where(key_mask[None, None, :], jnp.exp(scores), 0.0)
    numerator = jnp.einsum('hqk,khd->qhd', probs.astype(jnp.bfloat16).astype(jnp.float32), value_rows.astype(jnp.float32), precision=lax.Precision.HIGHEST)
    return (numerator, lax.optimization_barrier(jnp.sum(probs, axis=2)))

def reference(hidden_in, w_qkv, norm_gain, qk_gain, text_states, text_len, patch_len, stale_flags, stale_kv):
    width = HEADS * HEAD_DIM
    text_mask = jnp.arange(TEXT) < text_len[0]
    positions = jnp.arange(PATCH)
    state_all = hidden_in
    hidden_layers = []
    cache_layers = []
    for layer_idx in range(LAYERS):
        weight_flat = w_qkv[layer_idx].reshape(D, 3 * width)
        row_gain = norm_gain[layer_idx]
        query_gain = qk_gain[layer_idx, 0]
        key_gain = qk_gain[layer_idx, 1]
        text_normed = norm_rows(text_states[layer_idx].astype(jnp.float32), row_gain).astype(jnp.bfloat16)
        text_kv = jnp.dot(text_normed, weight_flat[:, width:], preferred_element_type=jnp.float32).astype(jnp.bfloat16)
        text_kv = text_kv.reshape(TEXT, 2, HEADS, HEAD_DIM)
        text_keys = norm_rows(text_kv[:, 0].astype(jnp.float32), key_gain).astype(jnp.bfloat16)
        text_values = text_kv[:, 1]
        layer_hidden = []
        layer_cache = []
        for micro_idx in range(MICRO):
            rows_in = state_all[micro_idx]
            normed = norm_rows(rows_in.astype(jnp.float32), row_gain).astype(jnp.bfloat16)
            projected = jnp.dot(normed, weight_flat, preferred_element_type=jnp.float32).reshape(PATCH, 3, width)
            fresh_kv = jnp.moveaxis(projected[:, 1:], 1, 0).astype(jnp.bfloat16)
            kept_kv = jnp.where(stale_flags[micro_idx, layer_idx] == 1, stale_kv[layer_idx, :, micro_idx], fresh_kv)
            key_rows = norm_rows(kept_kv[0].astype(jnp.float32).reshape(PATCH, HEADS, HEAD_DIM), key_gain).astype(jnp.bfloat16)
            value_rows = kept_kv[1].reshape(PATCH, HEADS, HEAD_DIM)
            queries = norm_rows(projected[:, 0].reshape(PATCH, HEADS, HEAD_DIM), query_gain).astype(jnp.bfloat16)
            text_num, text_den = attend_part(queries, text_keys, text_values, text_mask)
            own_num, own_den = attend_part(queries, key_rows, value_rows, positions < patch_len[micro_idx])
            attended = (text_num + own_num) / jnp.transpose(text_den + own_den)[:, :, None]
            layer_hidden.append((rows_in.astype(jnp.float32) + attended.reshape(PATCH, width)).astype(jnp.bfloat16))
            layer_cache.append(fresh_kv)
        state_all = jnp.stack(layer_hidden)
        hidden_layers.append(state_all)
        cache_layers.append(jnp.stack(layer_cache, axis=1))
    return (jnp.stack(hidden_layers), jnp.stack(cache_layers))
```

```python
import functools

import jax
import jax.numpy as jnp
from jax import lax
from jax.experimental import pallas as pl
from jax.experimental.pallas import tpu as pltpu
from jax.sharding import PartitionSpec as P

MESH = pl.DeviceIdType.MESH
F32 = jnp.float32
BF16 = jnp.bfloat16


def rms(values, gain):
    return values * lax.rsqrt(jnp.mean(values * values, axis=-1, keepdims=True) + 1e-06) * gain


def kernel(
    dims,
    text_len_in, patch_len_in, flags_in,
    hid_in, w_in, row_gain_in, head_gain_in, text_hbm, stale_in,
    hid_out, cache_out,
    text_len, patch_len, flags, row_gain, head_gain, ls,
    X, X1, RES, XN, text_in, TN, W, R, ST, TK, TV, hid_own, cache_own,
    all_in, clear, xs, xr, xfs, ws, wr, wrs, wcs, rr, fs, ss, sr,
    zs, zr, ys, yr, ms, mr, hs, hr, cs, cr, one,
):
    S, B, heads, hd, micro, tok = dims
    n = B // 2
    slots = (heads + 1) // 2
    rows = micro * tok
    total = B * rows
    width = heads * hd
    depth = w_in.shape[1]
    s, b, h = lax.axis_index("section"), lax.axis_index("blk"), lax.axis_index("head")
    first_owner = (B - heads) // 2
    off = first_owner - 1 + 2 * h if B - heads >= 2 else first_owner
    late = lax.rem(s, 2)
    pair = s + 1 - 2 * late
    mate = b + 1 - 2 * lax.rem(b, 2)
    my_half = b // n
    j_own = b - off
    owner = (b >= off) & (b < off + heads)
    half = pl.ds(pl.multiple_of(h * width, hd), width)
    other_half = pl.ds(pl.multiple_of((1 - h) * width, hd), width)

    def ahead(k):
        return lax.rem(b + k, B)

    def in_half(k):
        return my_half * n + lax.rem(b - my_half * n + k, n)

    def owns(c):
        return (c >= off) & (c < off + heads)

    def remote(src, dst, send, recv, dev):
        return pltpu.make_async_remote_copy(
            src_ref=src, dst_ref=dst, send_sem=send, recv_sem=recv, device_id=dev, device_id_type=MESH
        )

    def arrived(dst, sem):
        pltpu.make_async_copy(dst, dst, sem).wait()

    def sent(src, sem):
        remote(src, src, sem, sem, (s, b, 1 - h)).wait_send()

    def push(src, dst, send, recv, target):
        @pl.when(target == b)
        def _():
            pltpu.make_async_copy(src, dst, recv).start()

        @pl.when(target != b)
        def _():
            remote(src, dst, send, recv, (s, target, h)).start()

    def pushed(src, send, target):
        @pl.when(target != b)
        def _():
            sent(src, send)

    barrier = pltpu.get_barrier_semaphore()

    def hello(*dev):
        pl.semaphore_signal(barrier, inc=1, device_id=dev, device_id_type=MESH)

    across = lax.rem(b + n, B)
    for k in range(n):
        hello(pair, in_half(k), h)
    for k in range(1, n):
        hello(s, in_half(k), h)
    hello(s, b, 1 - h)
    hello(pair, across, h)
    hello(s, across, h)
    beside = jnp.where(late == 1, s + 1, s - 1)
    linked = (beside >= 0) & (beside < S)
    if S > 2:
        @pl.when(linked)
        def _():
            for k in range(0, B, 2):
                hello(beside, ahead(k), h)

    text_copy = pltpu.make_async_copy(text_hbm, text_in, one.at[5])
    text_copy.start()
    small = (
        (text_len_in, text_len), (patch_len_in, patch_len), (flags_in, flags),
        (row_gain_in, row_gain), (head_gain_in, head_gain),
    )
    loads = [pltpu.make_async_copy(src, dst, ls.at[i]) for i, (src, dst) in enumerate(small)]
    for load in loads:
        load.start()

    def row_block(c):
        return X.at[c, :, half]

    def col_block(j):
        return X1.at[h, j]

    @pl.when(s == 0)
    def _():
        pltpu.make_async_copy(hid_in, row_block(b), one.at[2]).start()

    with jax.named_scope("barrier"):
        pl.semaphore_wait(barrier, 2 * n + 2 + (linked.astype(jnp.int32) * n if S > 2 else 0))

    pl.semaphore_signal(all_in, inc=1, device_id=(s, across, h), device_id_type=MESH)

    @pl.when(s == 0)
    def _():
        remote(hid_in, row_block(b), xfs.at[0], xr.at[b], (s, mate, h)).start()

    def send_states(which):
        for k in range(2, B, 2):
            @pl.when((s == 1) & which(ahead(k)))
            def _():
                remote(hid_in, row_block(b), xs.at[k // 2], xr.at[b], (s - 1, ahead(k), h)).start()

    def cols_of(j):
        return pl.ds(pl.multiple_of(j * hd, hd), hd)

    def w_cols(j):
        return w_in.at[:, :, cols_of(j)]

    def w_rows(c):
        return W.at[:, pl.ds(pl.multiple_of(c * depth, depth), depth), :]

    def odd_head(c, t):
        return 2 * t + lax.rem(c + off + 1, 2)

    def even_head(c, t):
        return 2 * t + lax.rem(c + off, 2)

    def crosses(c, j):
        return (j < heads) & ((j + off) // n != c // n)

    def stays(j):
        return (j + off) // n == my_half

    def send_relayed():
        for t in range(slots):
            j = odd_head(b, t)

            @pl.when(crosses(b, j))
            def _():
                via = jnp.where(late == 1, b, mate)
                remote(w_cols(j), R.at[t], wrs.at[t], rr.at[t], (pair, via, h)).start()

    def near(c):
        return (c // n == my_half) | (c == across)

    def far(c):
        return jnp.logical_not(near(c))

    def send_crossing(which):
        for t in range(slots):
            j = even_head(b, t)

            @pl.when(crosses(b, j) & which(j + off))
            def _():
                remote(w_cols(j), w_rows(b), wcs.at[t], wr.at[b], (s, j + off, h)).start()

    def send_staying():
        for k in range(heads):
            j = lax.rem(b + k, heads)

            @pl.when(stays(j))
            def _():
                push(w_cols(j), w_rows(b), ws.at[k], wr.at[b], j + off)

    def send_stale(which):
        for k in range(heads):
            j = lax.rem(b + k, heads)

            @pl.when(which(j + off))
            def _():
                push(stale_in.at[:, :, cols_of(j)], ST.at[:, b], ss.at[k], sr.at[b], j + off)

    def sends_done():
        for t in range(slots):
            @pl.when(crosses(b, odd_head(b, t)))
            def _():
                sent(w_cols(0), wrs.at[t])

            @pl.when(crosses(b, even_head(b, t)))
            def _():
                sent(w_cols(0), wcs.at[t])

        for k in range(heads):
            j = lax.rem(b + k, heads)

            @pl.when(stays(j))
            def _():
                pushed(w_cols(j), ws.at[k], j + off)

            pushed(stale_in.at[:, :, cols_of(j)], ss.at[k], j + off)

    cb = jnp.where(late == 1, mate, b)

    def relayed(t):
        j = odd_head(cb, t)
        return crosses(cb, j), remote(R.at[t], w_rows(cb), fs.at[t], wr.at[cb], (pair, j + off, h))

    def relay():
        for t in range(slots):
            used, onward = relayed(t)

            @pl.when(used)
            def _():
                arrived(R.at[t], rr.at[t])
                onward.start()

    def relay_done():
        for t in range(slots):
            used, _ = relayed(t)

            @pl.when(used)
            def _():
                sent(R.at[t], fs.at[t])

    def all_clear():
        for k in range(2, n, 2):
            pl.semaphore_signal(clear, inc=1, device_id=(s, in_half(k), h), device_id_type=MESH)
        with jax.named_scope("clear"):
            pl.semaphore_wait(clear, n // 2 - 1)

    inner = lax.rem(b, n) // (n // 2) != my_half
    outer = jnp.logical_not(inner)
    early = late == 0

    send_states(near)

    @pl.when(early)
    def _():
        send_relayed()
        send_stale(near)

    @pl.when(inner)
    def _():
        send_crossing(near)

    @pl.when(early & outer)
    def _():
        send_staying()

    with jax.named_scope("all_in"):
        pl.semaphore_wait(all_in, 1)

    send_states(far)

    @pl.when(early)
    def _():
        @pl.when(inner)
        def _():
            send_crossing(far)

        @pl.when(outer)
        def _():
            send_crossing(near)
            send_crossing(far)

        send_stale(far)

        @pl.when(inner)
        def _():
            send_staying()

    @pl.when(s == 0)
    def _():
        with jax.named_scope("xcol"):
            for k in range(2, B, 2):
                c = ahead(k)
                arrived(row_block(c), xr.at[c])
                remote(row_block(c), row_block(c), xfs.at[k // 2], xr.at[c], (s, mate, h)).start()

    for load in loads:
        load.wait()
    text_copy.wait()

    @pl.when(owner)
    def _():
        TN[...] = rms(text_in[...].astype(F32), row_gain[...]).astype(BF16)

    @pl.when(late == 1)
    def _():
        with jax.named_scope("relay"):
            relay()
        with jax.named_scope("relay_done"):
            relay_done()
        send_relayed()
        all_clear()


        @pl.when(outer)
        def _():
            send_staying()
            send_crossing(near)

        send_crossing(far)

        @pl.when(inner)
        def _():
            send_staying()

        send_stale(near)
        send_stale(far)

    def norm_states(values):
        values = values.astype(F32)
        XN[...] = rms(values, row_gain[...]).astype(BF16)

    def swap_cores():
        return remote(X.at[:, :, half], X.at[:, :, half], one.at[0], one.at[1], (s, b, 1 - h))

    @pl.when(s == 0)
    def _():
        with jax.named_scope("waitX"):
            pltpu.make_async_copy(hid_in, row_block(b), one.at[2]).wait()
            for k in range(0, B, 2):
                c = lax.rem(mate + k, B)
                arrived(row_block(c), xr.at[c])

        swap_cores().start()
        with jax.named_scope("waitswap"):
            arrived(X.at[:, :, other_half], one.at[1])

        @pl.when(owner)
        def _():
            norm_states(X[...].reshape(total, 2 * width))
            RES[...] = X[:, :, pl.ds(pl.multiple_of(h * width + j_own * hd, hd), hd)].reshape(total, hd)

    @pl.when(early)
    def _():
        with jax.named_scope("relay"):
            relay()

    def to_core(c, k):
        return remote(col_block(c - off), col_block(c - off), ms.at[k], mr.at[c - off], (s, b, 1 - h))

    @pl.when(s > 0)
    def _():
        with jax.named_scope("waitX1"):
            for k in range(0, B, 2):
                c = ahead(k)

                @pl.when(owns(c))
                def _():
                    block = col_block(c - off)
                    arrived(block, zr.at[c])
                    remote(block, block, ys.at[k], yr.at[c], (s, mate, h)).start()
                    to_core(c, k).start()

        with jax.named_scope("waitX1m"):
            for k in range(0, B, 2):
                c = lax.rem(mate + k, B)

                @pl.when(owns(c))
                def _():
                    arrived(col_block(c - off), yr.at[c])
                    to_core(c, k + 1).start()

        with jax.named_scope("waitX1c"):
            for j in range(heads):
                arrived(X1.at[1 - h, j], mr.at[j])

        @pl.when(owner)
        def _():
            norm_states(
                jnp.concatenate([X1[i, j] for i in range(2) for j in range(heads)], axis=1)
            )
            RES[...] = X1[h, j_own]

    @pl.when(owner)
    def _():
        with jax.named_scope("waitW"):
            for c in range(B):
                arrived(W.at[:, pl.ds(c * depth, depth), :], wr.at[c])
        text_kv = jnp.dot(
            TN[...], jnp.concatenate([W[1], W[2]], axis=1), preferred_element_type=F32
        ).astype(BF16)
        TK[...] = rms(text_kv[:, :hd].astype(F32), head_gain[1:2, :]).astype(BF16)
        TV[...] = text_kv[:, hd:]
        proj = jnp.dot(
            XN[...], jnp.concatenate([W[0], W[1], W[2]], axis=1), preferred_element_type=F32
        )
        fresh_k = proj[:, hd : 2 * hd].astype(BF16)
        fresh_v = proj[:, 2 * hd :].astype(BF16)
        cache_own[0] = fresh_k.reshape(B, rows, hd)
        cache_own[1] = fresh_v.reshape(B, rows, hd)
        cols = cols_of(j_own)

        def push_cache():
            for k in range(B):
                t = ahead(k)
                push(cache_own.at[:, t], cache_out.at[:, :, cols], cs.at[k], cr.at[j_own], t)

        @pl.when(s == S - 1)
        def _():
            push_cache()

        with jax.named_scope("waitST"):
            for c in range(B):
                arrived(ST.at[:, c], sr.at[c])
        tok_bits = tok.bit_length() - 1

        def place(shape, axis):
            at = lax.broadcasted_iota(jnp.int32, shape, axis)
            which = lax.shift_right_logical(at, tok_bits) & (micro - 1)
            spot = lax.shift_right_logical(at, rows.bit_length() - 1) * tok + (at & (tok - 1))
            return which, spot

        def per_micro(which, read):
            out = jnp.zeros(which.shape, jnp.int32)
            for m in range(micro):
                out = jnp.where(which == m, read(m), out)
            return out

        which, _ = place((total, hd), 0)
        use_stale = per_micro(which, lambda m: flags[s, m]) == 1
        kept_k = jnp.where(use_stale, ST[0].reshape(total, hd).astype(F32), fresh_k.astype(F32))
        kept_v = jnp.where(use_stale, ST[1].reshape(total, hd).astype(F32), fresh_v.astype(F32))
        keys = rms(kept_k, head_gain[1:2, :]).astype(BF16)
        queries = rms(proj[:, :hd], head_gain[0:1, :]).astype(BF16)
        scale = hd**-0.5
        nt = (((1,), (1,)), ((), ()))

        def attend(key_rows, value_rows, mask):
            scores = lax.dot_general(queries, key_rows, nt, preferred_element_type=F32) * scale
            probs = jnp.where(mask, jnp.exp(scores), 0.0)
            num = jnp.dot(probs.astype(BF16), value_rows, preferred_element_type=F32)
            return num, jnp.sum(probs, axis=1, keepdims=True)

        shape = (total, total)
        q_which, _ = place(shape, 0)
        k_which, k_spot = place(shape, 1)
        mask = (q_which == k_which) & (k_spot < per_micro(k_which, lambda m: patch_len[m]))
        num, den = attend(keys, kept_v.astype(BF16), mask)
        text_at = lax.broadcasted_iota(jnp.int32, (total, TK.shape[0]), 1)
        text_num, text_den = attend(TK[...], TV[...], text_at < text_len[0])
        attended = (num + text_num) / (den + text_den)
        hid_own[...] = (RES[...].astype(F32) + attended).astype(BF16)

        @pl.when(s < S - 1)
        def _():
            for k in range(0, B, 2):
                remote(hid_own, col_block(j_own), zs.at[k], zr.at[b], (s + 1, ahead(k), h)).start()

        @pl.when(s < S - 1)
        def _():
            for k in range(0, B, 2):
                sent(hid_own, zs.at[k])

        for k in range(B):
            t = ahead(k)
            push(hid_own.at[pl.ds(pl.multiple_of(t * rows, rows), rows), :], hid_out.at[:, cols], hs.at[k], hr.at[j_own], t)
        @pl.when(s < S - 1)
        def _():
            push_cache()

    with jax.named_scope("waitOut"):
        for j in range(heads):
            cols = pl.ds(j * hd, hd)
            arrived(hid_out.at[:, cols], hr.at[j])
            arrived(cache_out.at[:, :, cols], cr.at[j])

    @pl.when(owner)
    def _():
        for k in range(B):
            t = ahead(k)
            pushed(hid_own.at[pl.ds(0, rows), :], hs.at[k], t)
            pushed(cache_own.at[:, t], cs.at[k], t)

    sends_done()

    @pl.when(late == 0)
    def _():
        relay_done()

    @pl.when(s == 0)
    def _():
        swap_cores().wait_send()
        for k in range(n):
            sent(hid_in, xfs.at[k])

    @pl.when(s == 1)
    def _():
        for k in range(1, n):
            sent(hid_in, xs.at[k])

    @pl.when(s > 0)
    def _():
        block = col_block(0)
        for k in range(0, B, 2):
            @pl.when(owns(ahead(k)))
            def _():
                sent(block, ys.at[k])
                sent(block, ms.at[k])

            @pl.when(owns(lax.rem(mate + k, B)))
            def _():
                sent(block, ms.at[k + 1])


def shards(
    hidden_in, w_qkv, norm_gain, qk_gain, text_states, text_len, patch_len, stale_flags, stale_kv
):
    S, B = lax.axis_size("section"), lax.axis_size("blk")
    micro, tok, width = hidden_in.shape
    hd = qk_gain.shape[2]
    heads = width // hd
    rows = micro * tok
    total = B * rows
    depth = w_qkv.shape[1]
    text = text_states.shape[1]
    n, slots = B // 2, (heads + 1) // 2
    w = w_qkv[0].transpose(1, 0, 2)
    vmem = pl.BlockSpec(memory_space=pltpu.VMEM)
    hbm = pl.BlockSpec(memory_space=pltpu.HBM)
    sem = pltpu.SemaphoreType.DMA
    hid, cache = pl.pallas_call(
        functools.partial(kernel, (S, B, heads, hd, micro, tok)),
        out_shape=(
            pltpu.VMEM((rows, width), BF16),
            pltpu.VMEM((2, rows, width), BF16),
        ),
        in_specs=[hbm] * 9,
        out_specs=(vmem, vmem),
        scratch_shapes=[
            pltpu.SMEM(text_len.shape, jnp.int32),
            pltpu.SMEM(patch_len.shape, jnp.int32),
            pltpu.SMEM(stale_flags.shape[::-1], jnp.int32),
            pltpu.VMEM(norm_gain.shape, F32),
            pltpu.VMEM(qk_gain.shape[1:], F32),
            sem((5,)),
            pltpu.VMEM((B, rows, 2 * width), BF16),
            pltpu.VMEM((2, heads, total, hd), BF16),
            pltpu.VMEM((total, hd), BF16),
            pltpu.VMEM((total, 2 * width), BF16),
            pltpu.VMEM((text, 2 * width), BF16),
            pltpu.VMEM((text, 2 * width), BF16),
            pltpu.VMEM((3, B * depth, hd), BF16),
            pltpu.VMEM((slots, 3, depth, hd), BF16),
            pltpu.VMEM((2, B, rows, hd), BF16),
            pltpu.VMEM((text, hd), BF16),
            pltpu.VMEM((text, hd), BF16),
            pltpu.VMEM((total, hd), BF16),
            pltpu.VMEM((2, B, rows, hd), BF16),
            pltpu.SemaphoreType.REGULAR, pltpu.SemaphoreType.REGULAR,
            sem((n,)), sem((B,)), sem((n,)),
            sem((heads,)), sem((B,)), sem((slots,)), sem((slots,)), sem((slots,)), sem((slots,)),
            sem((heads,)), sem((B,)),
            sem((B,)), sem((B,)), sem((B,)), sem((B,)), sem((B,)), sem((heads,)),
            sem((B,)), sem((heads,)), sem((B,)), sem((heads,)),
            sem((6,)),
        ],
        compiler_params=pltpu.CompilerParams(
            collective_id=0, has_side_effects=True, vmem_limit_bytes=60 * 1024 * 1024
        ),
    )(
        text_len, patch_len, stale_flags.T,
        hidden_in.reshape(rows, width), w, norm_gain, qk_gain[0], text_states[0],
        stale_kv[0].reshape(2, rows, width),
    )
    return (
        hid.reshape(1, micro, tok, width),
        cache.reshape(1, 2, micro, tok, width),
    )


def solution(mesh):
    in_specs = (
        P(None, "blk", "head"),
        P("section", "blk", None, "head"),
        P("section", None),
        P("section", None, None),
        P("section", None, None),
        P(),
        P(),
        P(),
        P("section", None, None, "blk", "head"),
    )
    out_specs = (P("section", None, "blk", "head"), P("section", None, None, "blk", "head"))
    return jax.shard_map(shards, mesh=mesh, in_specs=in_specs, out_specs=out_specs, check_vma=False)
```

```python
import functools

import jax
import jax.numpy as jnp
from jax import lax
from jax.experimental import pallas as pl
from jax.experimental.pallas import tpu as pltpu
from jax.sharding import PartitionSpec as P

MESH = pl.DeviceIdType.MESH
F32 = jnp.float32
BF16 = jnp.bfloat16


def rms(values, gain):
    return values * lax.rsqrt(jnp.mean(values * values, axis=-1, keepdims=True) + 1e-06) * gain


def kernel(
    dims,
    text_len_in, patch_len_in, flags_in,
    hid_in, w_in, row_gain_in, head_gain_in, text_hbm, stale_in,
    hid_out, cache_out,
    text_len, patch_len, flags, row_gain, head_gain,
    X, X1, RES, XN, text_in, TN, W, R, PROJ, TKV, ST, TK, TV,
    hid_own, cache_own,
    all_in, clear, ls, xr, zs, zr, yr, rr, fs, one,
):
    S, B, heads, hd, micro, tok = dims
    n = B // 2
    slots = (heads + 1) // 2
    rows = micro * tok
    total = B * rows
    width = heads * hd
    depth = w_in.shape[1]
    s, b, h = lax.axis_index("section"), lax.axis_index("blk"), lax.axis_index("head")
    first_owner = (B - heads) // 2
    off = first_owner - 1 + 2 * h if B - heads >= 2 else first_owner
    late = lax.rem(s, 2)
    early = late == 0
    pair = s + 1 - 2 * late
    mate = b + 1 - 2 * lax.rem(b, 2)
    my_half = b // n
    across = lax.rem(b + n, B)
    inner = lax.rem(b, n) // (n // 2) != my_half
    outer = jnp.logical_not(inner)
    j_own = b - off
    owner = (b >= off) & (b < off + heads)
    core = (s, b, 1 - h)
    half = pl.ds(pl.multiple_of(h * width, hd), width)
    other_half = pl.ds(pl.multiple_of((1 - h) * width, hd), width)
    (
        w_send, w_recv, st_send, st_recv, x_send, xm_send, xc_send, xc_recv, x_own, text_recv,
        ym_send, core_send, core_recv, hid_send, hid_recv, cache_send, cache_recv,
    ) = [one.at[i] for i in range(17)]

    def ahead(k):
        return lax.rem(b + k, B)

    def in_half(k):
        return my_half * n + lax.rem(b - my_half * n + k, n)

    def nearest(k):
        return in_half(k) if k < n else lax.rem(in_half(k - n) + n, B)

    def owns(c):
        return (c >= off) & (c < off + heads)

    def near(c):
        return (c // n == my_half) | (c == across)

    def far(c):
        return jnp.logical_not(near(c))

    def remote(src, dst, send, recv, dev):
        return pltpu.make_async_remote_copy(
            src_ref=src, dst_ref=dst, send_sem=send, recv_sem=recv, device_id=dev, device_id_type=MESH
        )

    def arrived(dst, sem):
        pltpu.make_async_copy(dst, dst, sem).wait()

    def sent(src, sem):
        remote(src, src, sem, sem, core).wait_send()

    def push(src, dst, send, recv, target):
        @pl.when(target == b)
        def _():
            pltpu.make_async_copy(src, dst, recv).start()

        @pl.when(target != b)
        def _():
            remote(src, dst, send, recv, (s, target, h)).start()

    def cols_of(j):
        return pl.ds(pl.multiple_of(j * hd, hd), hd)

    def w_cols(j):
        return w_in.at[:, :, cols_of(j)]

    def w_rows(c):
        return W.at[:, pl.ds(pl.multiple_of(c * depth, depth), depth), :]

    def row_block(c):
        return X.at[c, :, half]

    barrier = pltpu.get_barrier_semaphore()

    def hello(*dev):
        pl.semaphore_signal(barrier, inc=1, device_id=dev, device_id_type=MESH)

    for k in range(n):
        hello(pair, in_half(k), h)
    for k in range(1, n):
        hello(s, in_half(k), h)
    hello(*core)
    hello(pair, across, h)
    hello(s, across, h)
    beside = jnp.where(late == 1, s + 1, s - 1)
    linked = (beside >= 0) & (beside < S)
    if S > 2:
        @pl.when(linked)
        def _():
            for k in range(0, B, 2):
                hello(beside, ahead(k), h)

    text_copy = pltpu.make_async_copy(text_hbm, text_in, text_recv)
    text_copy.start()
    small = (
        (text_len_in, text_len), (patch_len_in, patch_len), (flags_in, flags),
        (row_gain_in, row_gain), (head_gain_in, head_gain),
    )
    loads = [pltpu.make_async_copy(src, dst, ls.at[i]) for i, (src, dst) in enumerate(small)]
    for load in loads:
        load.start()

    @pl.when(s == 0)
    def _():
        pltpu.make_async_copy(hid_in, row_block(b), x_own).start()

    for load in loads:
        load.wait()
    text_copy.wait()
    TN[...] = rms(text_in[...].astype(F32), row_gain[...]).astype(BF16)

    with jax.named_scope("barrier"):
        pl.semaphore_wait(barrier, 2 * n + 2 + (linked.astype(jnp.int32) * n if S > 2 else 0))

    pl.semaphore_signal(all_in, inc=1, device_id=(s, across, h), device_id_type=MESH)

    def other_side(c, t):
        return 2 * t + lax.rem(c + off + 1, 2)

    def same_side(c, t):
        return 2 * t + lax.rem(c + off, 2)

    def crosses(c, j):
        return (j < heads) & ((j + off) // n != c // n)

    def send_relayed():
        for t in range(slots):
            j = other_side(b, t)

            @pl.when(crosses(b, j))
            def _():
                via = jnp.where(late == 1, b, mate)
                remote(w_cols(j), R.at[t], w_send, rr.at[t], (pair, via, h)).start()

    def send_crossing(which):
        for t in range(slots):
            j = same_side(b, t)

            @pl.when(crosses(b, j) & which(j + off))
            def _():
                remote(w_cols(j), w_rows(b), w_send, w_recv, (s, j + off, h)).start()

    def send_staying():
        for k in range(heads):
            j = lax.rem(b + k, heads)

            @pl.when((j + off) // n == my_half)
            def _():
                push(w_cols(j), w_rows(b), w_send, w_recv, j + off)

    def send_stale(which):
        for k in range(heads):
            j = lax.rem(b + k, heads)

            @pl.when(which(j + off))
            def _():
                push(stale_in.at[:, :, cols_of(j)], ST.at[:, b], st_send, st_recv, j + off)

    cb = jnp.where(late == 1, mate, b)

    def relayed(t):
        j = other_side(cb, t)
        return crosses(cb, j), remote(R.at[t], w_rows(cb), fs.at[t], w_recv, (pair, j + off, h))

    def relay():
        for t in range(slots):
            used, onward = relayed(t)

            @pl.when(used)
            def _():
                arrived(R.at[t], rr.at[t])
                onward.start()

    def relay_done():
        for t in range(slots):
            used, _ = relayed(t)

            @pl.when(used)
            def _():
                sent(R.at[t], fs.at[t])

    def send_states(which):
        for k in range(2, B, 2):
            @pl.when(which(nearest(k)))
            def _():
                remote(hid_in, row_block(b), x_send, xr.at[b], (s - 1, nearest(k), h)).start()

    def block_to_core(c):
        return remote(row_block(c), row_block(c), xc_send, xc_recv, core)

    @pl.when(s == 1)
    def _():
        send_states(near)

    @pl.when(early)
    def _():
        send_relayed()

        @pl.when(s == 0)
        def _():
            pltpu.make_async_copy(hid_in, row_block(b), x_own).wait()
            remote(row_block(b), row_block(b), xm_send, xr.at[b], (s, mate, h)).start()
            block_to_core(b).start()

        send_stale(near)

        @pl.when(inner)
        def _():
            send_crossing(near)

    with jax.named_scope("all_in"):
        pl.semaphore_wait(all_in, 1)

    @pl.when(early)
    def _():
        send_stale(far)

        @pl.when(outer)
        def _():
            send_crossing(near)

        send_crossing(far)

        @pl.when(s == 0)
        def _():
            with jax.named_scope("xcol"):
                for k in range(2, B, 2):
                    c = nearest(k)
                    arrived(row_block(c), xr.at[c])
                    remote(row_block(c), row_block(c), xm_send, xr.at[c], (s, mate, h)).start()
                    block_to_core(c).start()

        send_staying()

    @pl.when(late == 1)
    def _():
        @pl.when(s == 1)
        def _():
            send_states(far)

        send_relayed()
        with jax.named_scope("relay"):
            relay()
        with jax.named_scope("relay_done"):
            relay_done()
        for k in range(2, n, 2):
            pl.semaphore_signal(clear, inc=1, device_id=(s, in_half(k), h), device_id_type=MESH)
        send_staying()
        with jax.named_scope("clear"):
            pl.semaphore_wait(clear, n // 2 - 1)
        send_crossing(near)
        send_crossing(far)
        send_stale(near)
        send_stale(far)

    def norm_states(values):
        XN[...] = rms(values.astype(F32), row_gain[...]).astype(BF16)

    @pl.when(s == 0)
    def _():
        with jax.named_scope("waitX"):
            for k in range(0, B, 2):
                c = nearest(k) + mate - b
                arrived(row_block(c), xr.at[c])
                block_to_core(c).start()
        with jax.named_scope("waitswap"):
            arrived(X.at[:, :, other_half], xc_recv)

        @pl.when(owner)
        def _():
            norm_states(X[...].reshape(total, 2 * width))
            RES[...] = X[:, :, pl.ds(pl.multiple_of(h * width + j_own * hd, hd), hd)]

    @pl.when(early & jnp.logical_not(owner))
    def _():
        with jax.named_scope("relayW1"):
            relay()

    def col_block(j):
        return X1.at[h, j]

    def to_core(c):
        return remote(col_block(c - off), col_block(c - off), core_send, core_recv, core)

    @pl.when(s > 0)
    def _():
        with jax.named_scope("waitX1"):
            for k in range(0, B, 2):
                c = nearest(k)

                @pl.when(owns(c))
                def _():
                    block = col_block(c - off)
                    arrived(block, zr.at[c - off])
                    remote(block, block, ym_send, yr.at[c - off], (s, mate, h)).start()
                    to_core(c).start()

        with jax.named_scope("waitX1m"):
            for k in range(0, B, 2):
                c = nearest(k) + mate - b

                @pl.when(owns(c))
                def _():
                    arrived(col_block(c - off), yr.at[c - off])
                    to_core(c).start()

        with jax.named_scope("waitX1c"):
            arrived(X1.at[1 - h], core_recv)

        @pl.when(owner)
        def _():
            norm_states(jnp.concatenate([X1[i, j] for i in range(2) for j in range(heads)], axis=1))
            RES[...] = X1[h, j_own].reshape(RES.shape)

    @pl.when(owner)
    def _():
        with jax.named_scope("waitW"):
            arrived(W, w_recv)
        w_kv = jnp.concatenate([W[1], W[2]], axis=1)
        TKV[...] = jnp.dot(TN[...], w_kv, preferred_element_type=F32).astype(BF16)
        PROJ[...] = jnp.dot(
            XN[...], jnp.concatenate([W[0], w_kv], axis=1), preferred_element_type=F32
        )

    @pl.when(owner)
    def _():
        fresh_k = PROJ[:, hd : 2 * hd].astype(BF16)
        fresh_v = PROJ[:, 2 * hd :].astype(BF16)
        cache_own[0] = fresh_k.reshape(B, rows, hd)
        cache_own[1] = fresh_v.reshape(B, rows, hd)
        cols = cols_of(j_own)

        def push_cache():
            for k in range(B):
                t = ahead(k)
                push(cache_own.at[:, t], cache_out.at[:, :, cols], cache_send, cache_recv, t)

        @pl.when(s == S - 1)
        def _():
            push_cache()

        TK[...] = rms(TKV[:, :hd].astype(F32), head_gain[1:2, :]).astype(BF16)
        TV[...] = TKV[:, hd:]
        with jax.named_scope("waitST"):
            arrived(ST, st_recv)
        tok_bits = tok.bit_length() - 1

        def place(shape, axis):
            at = lax.broadcasted_iota(jnp.int32, shape, axis)
            which = lax.shift_right_logical(at, tok_bits) & (micro - 1)
            spot = lax.shift_right_logical(at, rows.bit_length() - 1) * tok + (at & (tok - 1))
            return which, spot

        def per_micro(which, read):
            out = jnp.zeros(which.shape, jnp.int32)
            for m in range(micro):
                out = jnp.where(which == m, read(m), out)
            return out

        which, _ = place((total, hd), 0)
        use_stale = per_micro(which, lambda m: flags[s, m]) == 1
        kept_k = jnp.where(use_stale, ST[0].reshape(total, hd).astype(F32), fresh_k.astype(F32))
        kept_v = jnp.where(use_stale, ST[1].reshape(total, hd).astype(F32), fresh_v.astype(F32))
        keys = rms(kept_k, head_gain[1:2, :]).astype(BF16)
        queries = rms(PROJ[:, :hd], head_gain[0:1, :]).astype(BF16)
        scale = hd**-0.5
        nt = (((1,), (1,)), ((), ()))

        def attend(key_rows, value_rows, mask):
            scores = lax.dot_general(queries, key_rows, nt, preferred_element_type=F32) * scale
            probs = jnp.where(mask, jnp.exp(scores), 0.0)
            num = jnp.dot(probs.astype(BF16), value_rows, preferred_element_type=F32)
            return num, jnp.sum(probs, axis=1, keepdims=True)

        shape = (total, total)
        q_which, _ = place(shape, 0)
        k_which, k_spot = place(shape, 1)
        mask = (q_which == k_which) & (k_spot < per_micro(k_which, lambda m: patch_len[m]))
        num, den = attend(keys, kept_v.astype(BF16), mask)
        text_at = lax.broadcasted_iota(jnp.int32, (total, TK.shape[0]), 1)
        text_num, text_den = attend(TK[...], TV[...], text_at < text_len[0])
        attended = (num + text_num) / (den + text_den)
        hid_own[...] = (RES[...].reshape(total, hd).astype(F32) + attended).astype(BF16)

        @pl.when(s < S - 1)
        def _():
            for k in range(0, B, 2):
                remote(hid_own, col_block(j_own), zs.at[k // 2], zr.at[j_own], (s + 1, ahead(k), h)).start()

        @pl.when(early)
        def _():
            relay()

        @pl.when(s < S - 1)
        def _():
            for k in range(0, B, 2):
                sent(hid_own, zs.at[k // 2])

        for k in range(B):
            t = ahead(k)
            push(hid_own.at[pl.ds(pl.multiple_of(t * rows, rows), rows), :], hid_out.at[:, cols], hid_send, hid_recv, t)
        @pl.when(s < S - 1)
        def _():
            push_cache()

    with jax.named_scope("waitOut"):
        arrived(hid_out, hid_recv)
        arrived(cache_out, cache_recv)

    @pl.when(owner)
    def _():
        sent(hid_own.at[pl.ds(0, total - rows), :], hid_send)
        sent(cache_own.at[:, pl.ds(0, B - 1)], cache_send)
        sent(w_in.at[:, :, pl.ds(0, width - hd)], w_send)
        sent(stale_in.at[:, :, pl.ds(0, width - hd)], st_send)

    @pl.when(jnp.logical_not(owner))
    def _():
        sent(w_in, w_send)
        sent(stale_in, st_send)

    @pl.when(early)
    def _():
        relay_done()

    @pl.when(s == 0)
    def _():
        sent(X.at[pl.ds(0, n), :, half], xm_send)
        sent(X.at[:, :, half], xc_send)

    @pl.when(s == 1)
    def _():
        sent(X.at[pl.ds(0, n - 1), :, half], x_send)

    @pl.when(s > 0)
    def _():
        sent(X1.at[h, pl.ds(0, heads // 2)], ym_send)
        sent(X1.at[h], core_send)


def shards(
    hidden_in, w_qkv, norm_gain, qk_gain, text_states, text_len, patch_len, stale_flags, stale_kv
):
    S, B = lax.axis_size("section"), lax.axis_size("blk")
    micro, tok, width = hidden_in.shape
    hd = qk_gain.shape[2]
    heads = width // hd
    rows = micro * tok
    total = B * rows
    depth = w_qkv.shape[1]
    text = text_states.shape[1]
    n, slots = B // 2, (heads + 1) // 2
    w = w_qkv[0].transpose(1, 0, 2)
    hbm = pl.BlockSpec(memory_space=pltpu.HBM)
    sem = pltpu.SemaphoreType.DMA
    hid, cache = pl.pallas_call(
        functools.partial(kernel, (S, B, heads, hd, micro, tok)),
        out_shape=(
            pltpu.VMEM((rows, width), BF16),
            pltpu.VMEM((2, rows, width), BF16),
        ),
        in_specs=[hbm] * 9,
        out_specs=(pl.BlockSpec(memory_space=pl.ANY),) * 2,
        scratch_shapes=[
            pltpu.SMEM(text_len.shape, jnp.int32),
            pltpu.SMEM(patch_len.shape, jnp.int32),
            pltpu.SMEM(stale_flags.shape[::-1], jnp.int32),
            pltpu.VMEM(norm_gain.shape, F32),
            pltpu.VMEM(qk_gain.shape[1:], F32),
            pltpu.VMEM((B, rows, 2 * width), BF16),
            pltpu.VMEM((2, heads, total, hd), BF16),
            pltpu.VMEM((B, rows, hd), BF16),
            pltpu.VMEM((total, 2 * width), BF16),
            pltpu.VMEM((text, 2 * width), BF16),
            pltpu.VMEM((text, 2 * width), BF16),
            pltpu.VMEM((3, B * depth, hd), BF16),
            pltpu.VMEM((slots, 3, depth, hd), BF16),
            pltpu.VMEM((total, 3 * hd), F32),
            pltpu.VMEM((text, 2 * hd), BF16),
            pltpu.VMEM((2, B, rows, hd), BF16),
            pltpu.VMEM((text, hd), BF16),
            pltpu.VMEM((text, hd), BF16),
            pltpu.VMEM((total, hd), BF16),
            pltpu.VMEM((2, B, rows, hd), BF16),
            pltpu.SemaphoreType.REGULAR, pltpu.SemaphoreType.REGULAR,
            sem((5,)), sem((B,)), sem((n,)), sem((heads,)), sem((heads,)),
            sem((slots,)), sem((slots,)), sem((17,)),
        ],
        compiler_params=pltpu.CompilerParams(
            collective_id=0, has_side_effects=True, vmem_limit_bytes=60 * 1024 * 1024
        ),
    )(
        text_len, patch_len, stale_flags.T,
        hidden_in.reshape(rows, width), w, norm_gain, qk_gain[0], text_states[0],
        stale_kv[0].reshape(2, rows, width),
    )
    return (
        hid.reshape(1, micro, tok, width),
        cache.reshape(1, 2, micro, tok, width),
    )


def solution(mesh):
    in_specs = (
        P(None, "blk", "head"),
        P("section", "blk", None, "head"),
        P("section", None),
        P("section", None, None),
        P("section", None, None),
        P(),
        P(),
        P(),
        P("section", None, None, "blk", "head"),
    )
    out_specs = (P("section", None, "blk", "head"), P("section", None, None, "blk", "head"))
    return jax.shard_map(shards, mesh=mesh, in_specs=in_specs, out_specs=out_specs, check_vma=False)
```

```python
import functools

import jax
import jax.numpy as jnp
from jax import lax
from jax.experimental import pallas as pl
from jax.experimental.pallas import tpu as pltpu
from jax.sharding import PartitionSpec as P

MESH = pl.DeviceIdType.MESH
F32 = jnp.float32
BF16 = jnp.bfloat16


def rms(values, gain):
    return values * lax.rsqrt(jnp.mean(values * values, axis=-1, keepdims=True) + 1e-06) * gain


def kernel(
    dims,
    text_len_in, patch_len_in, flags_in,
    hid_in, w_in, row_gain_in, head_gain_in, text_hbm, stale_in,
    hid_out, cache_out,
    text_len, patch_len, flags, row_gain, head_gain,
    X, X1, RES, XN, text_in, TN, W, R, PROJ, ST, TK, TV,
    hid_own, cache_own,
    all_in, clear, taken, ls, xr, zs, zr, yr, rr, fs, one,
):
    S, B, heads, hd, micro, tok = dims
    n = B // 2
    slots = (heads + 1) // 2
    rows = micro * tok
    total = B * rows
    width = heads * hd
    depth = w_in.shape[1]
    s, b, h = lax.axis_index("section"), lax.axis_index("blk"), lax.axis_index("head")
    first_owner = (B - heads) // 2
    off = first_owner - 1 + 2 * h if B - heads >= 2 else first_owner
    late = lax.rem(s, 2)
    early = late == 0
    pair = s + 1 - 2 * late
    mate = b + 1 - 2 * lax.rem(b, 2)
    my_half = b // n
    across = lax.rem(b + n, B)
    inner = lax.rem(b, n) // (n // 2) != my_half
    outer = jnp.logical_not(inner)
    j_own = b - off
    owner = (b >= off) & (b < off + heads)
    core = (s, b, 1 - h)
    half = pl.ds(pl.multiple_of(h * width, hd), width)
    other_half = pl.ds(pl.multiple_of((1 - h) * width, hd), width)
    (
        w_send, w_recv, st_send, st_recv, x_send, xm_send, xc_send, xc_recv, x_own, text_recv,
        ym_send, core_send, core_recv, hid_send, hid_recv, cache_send, cache_recv,
    ) = [one.at[i] for i in range(17)]

    def ahead(k):
        return lax.rem(b + k, B)

    def in_half(k):
        return my_half * n + lax.rem(b - my_half * n + k, n)

    def nearest(k):
        return in_half(k) if k < n else k + my_half * (2 * n - 2 - 2 * k) + lax.rem(b, 2)

    def owns(c):
        return (c >= off) & (c < off + heads)

    def near(c):
        return (c // n == my_half) | (c == across)

    def far(c):
        return jnp.logical_not(near(c))

    def remote(src, dst, send, recv, dev):
        return pltpu.make_async_remote_copy(
            src_ref=src, dst_ref=dst, send_sem=send, recv_sem=recv, device_id=dev, device_id_type=MESH
        )

    def arrived(dst, sem):
        pltpu.make_async_copy(dst, dst, sem).wait()

    def sent(src, sem):
        remote(src, src, sem, sem, core).wait_send()

    def push(src, dst, send, recv, target):
        @pl.when(target == b)
        def _():
            pltpu.make_async_copy(src, dst, recv).start()

        @pl.when(target != b)
        def _():
            remote(src, dst, send, recv, (s, target, h)).start()

    def cols_of(j):
        return pl.ds(pl.multiple_of(j * hd, hd), hd)

    def w_cols(j):
        return w_in.at[:, :, cols_of(j)]

    def w_rows(c):
        return W.at[:, pl.ds(pl.multiple_of(c * depth, depth), depth), :]

    def row_block(c):
        return X.at[c, :, half]

    barrier = pltpu.get_barrier_semaphore()

    def hello(*dev):
        pl.semaphore_signal(barrier, inc=1, device_id=dev, device_id_type=MESH)

    for k in range(n):
        hello(pair, in_half(k), h)
    for k in range(1, n):
        hello(s, in_half(k), h)
    hello(*core)
    hello(pair, across, h)
    hello(s, across, h)
    beside = jnp.where(late == 1, s + 1, s - 1)
    linked = (beside >= 0) & (beside < S)
    if S > 2:
        @pl.when(linked)
        def _():
            for k in range(0, B, 2):
                hello(beside, ahead(k), h)

    text_copy = pltpu.make_async_copy(text_hbm, text_in, text_recv)
    text_copy.start()
    small = (
        (text_len_in, text_len), (patch_len_in, patch_len), (flags_in, flags),
        (row_gain_in, row_gain), (head_gain_in, head_gain),
    )
    loads = [pltpu.make_async_copy(src, dst, ls.at[i]) for i, (src, dst) in enumerate(small)]
    for load in loads:
        load.start()

    @pl.when(s == 0)
    def _():
        pltpu.make_async_copy(hid_in, row_block(b), x_own).start()

    for load in loads:
        load.wait()
    text_copy.wait()
    TN[...] = rms(text_in[...].astype(F32), row_gain[...]).astype(BF16)

    with jax.named_scope("barrier"):
        pl.semaphore_wait(barrier, 2 * n + 2 + (linked.astype(jnp.int32) * n if S > 2 else 0))

    pl.semaphore_signal(all_in, inc=1, device_id=(s, across, h), device_id_type=MESH)

    def other_side(c, t):
        return 2 * t + lax.rem(c + off + 1, 2)

    def central(c):
        return lax.rem(c, n) // (n // 2) != c // n

    def crosses(c, j):
        return (j < heads) & ((j + off) // n != c // n)

    def detours(c, j):
        return crosses(c, j) & (lax.rem(j + off + c, 2) == 1)

    def send_relayed():
        for t in range(slots):
            j = other_side(b, t)

            @pl.when(detours(b, j))
            def _():
                remote(w_cols(j), R.at[t], w_send, rr.at[t], (pair, jnp.where(late == 1, b, mate), h)).start()

    def send_crossing(which):
        for k in range(heads):
            j = lax.rem(b + k, heads)

            @pl.when(crosses(b, j) & jnp.logical_not(detours(b, j)) & which(j + off))
            def _():
                remote(w_cols(j), w_rows(b), w_send, w_recv, (s, j + off, h)).start()

    def send_staying():
        for k in range(heads):
            j = lax.rem(b + k, heads)

            @pl.when((j + off) // n == my_half)
            def _():
                push(w_cols(j), w_rows(b), w_send, w_recv, j + off)

    def send_stale(which):
        for k in range(heads):
            j = lax.rem(b + k, heads)

            @pl.when(which(j + off))
            def _():
                push(stale_in.at[:, :, cols_of(j)], ST.at[:, b], st_send, st_recv, j + off)

    def relayed(t):
        cb = jnp.where(late == 1, mate, b)
        j = other_side(cb, t)
        return detours(cb, j), remote(R.at[t], w_rows(cb), fs.at[t], w_recv, (pair, j + off, h))

    def relay():
        for t in range(slots):
            used, onward = relayed(t)

            @pl.when(used)
            def _():
                arrived(R.at[t], rr.at[t])
                onward.start()

    def relay_done():
        for t in range(slots):
            used, _ = relayed(t)

            @pl.when(used)
            def _():
                sent(R.at[t], fs.at[t])

    def send_states(which):
        for k in range(2, B, 2):
            @pl.when(which(nearest(k)))
            def _():
                remote(hid_in, row_block(b), x_send, xr.at[b], (s - 1, nearest(k), h)).start()

    def block_to_core(c):
        return remote(row_block(c), row_block(c), xc_send, xc_recv, core)

    @pl.when(s == 1)
    def _():
        send_states(near)

    @pl.when(early)
    def _():
        send_relayed()

        @pl.when(s == 0)
        def _():
            pltpu.make_async_copy(hid_in, row_block(b), x_own).wait()
            remote(row_block(b), row_block(b), xm_send, xr.at[b], (s, mate, h)).start()
            block_to_core(b).start()

        send_stale(near)

        @pl.when(inner)
        def _():
            send_crossing(near)

    with jax.named_scope("all_in"):
        pl.semaphore_wait(all_in, 1)

    @pl.when(early)
    def _():
        send_stale(far)

        @pl.when(outer)
        def _():
            send_crossing(near)

        send_crossing(far)

        @pl.when(s == 0)
        def _():
            with jax.named_scope("xcol"):
                for k in range(2, B, 2):
                    c = nearest(k)
                    arrived(row_block(c), xr.at[c])
                    remote(row_block(c), row_block(c), xm_send, xr.at[c], (s, mate, h)).start()
                    block_to_core(c).start()

        send_staying()

    @pl.when(late == 1)
    def _():
        @pl.when(s == 1)
        def _():
            send_states(far)

        send_relayed()
        with jax.named_scope("relay"):
            relay()
        send_staying()
        with jax.named_scope("relay_done"):
            relay_done()
        for k in range(2, n, 2):
            pl.semaphore_signal(clear, inc=1, device_id=(s, in_half(k), h), device_id_type=MESH)
        with jax.named_scope("clear"):
            pl.semaphore_wait(clear, n // 2 - 1)
        send_crossing(near)
        send_crossing(far)
        send_stale(near)
        send_stale(far)

    def norm_states(values):
        XN[...] = rms(values.astype(F32), row_gain[...]).astype(BF16)

    @pl.when(s == 0)
    def _():
        with jax.named_scope("waitX"):
            for k in range(0, B, 2):
                c = nearest(k) + mate - b
                arrived(row_block(c), xr.at[c])
                block_to_core(c).start()
        with jax.named_scope("waitswap"):
            arrived(X.at[:, :, other_half], xc_recv)

        @pl.when(owner)
        def _():
            norm_states(X[...].reshape(total, 2 * width))
            RES[...] = X[:, :, pl.ds(pl.multiple_of(h * width + j_own * hd, hd), hd)]

    @pl.when(early & jnp.logical_not(owner))
    def _():
        with jax.named_scope("relayW1"):
            relay()

    def text_part():
        @pl.when(owner)
        def _():
            with jax.named_scope("waitW"):
                arrived(W, w_recv)
            text_kv = jnp.dot(
                TN[...], jnp.concatenate([W[1], W[2]], axis=1), preferred_element_type=F32
            ).astype(BF16)
            TK[...] = rms(text_kv[:, :hd].astype(F32), head_gain[1:2, :]).astype(BF16)
            TV[...] = text_kv[:, hd:]

    @pl.when(s == 0)
    def _():
        text_part()

    def col_block(j):
        return X1.at[h, j]

    def to_core(c):
        return remote(col_block(c - off), col_block(c - off), core_send, core_recv, core)

    @pl.when(s > 0)
    def _():
        with jax.named_scope("waitX1"):
            for k in range(0, B, 2):
                c = nearest(k)

                @pl.when(owns(c))
                def _():
                    block = col_block(c - off)
                    arrived(block, zr.at[c - off])
                    remote(block, block, ym_send, yr.at[c - off], (s, mate, h)).start()
                    to_core(c).start()

        pl.semaphore_signal(taken, inc=1, device_id=(s - 1, b, h), device_id_type=MESH)
        with jax.named_scope("waitX1m"):
            for k in range(0, B, 2):
                c = nearest(k) + mate - b

                @pl.when(owns(c))
                def _():
                    arrived(col_block(c - off), yr.at[c - off])
                    to_core(c).start()

        text_part()
        with jax.named_scope("waitX1c"):
            arrived(X1.at[1 - h], core_recv)

        @pl.when(owner)
        def _():
            norm_states(jnp.concatenate([X1[i, j] for i in range(2) for j in range(heads)], axis=1))
            RES[...] = X1[h, j_own].reshape(RES.shape)

    @pl.when(owner)
    def _():
        PROJ[...] = jnp.dot(
            XN[...], jnp.concatenate([W[0], W[1], W[2]], axis=1), preferred_element_type=F32
        )

    def push_cache():
        for k in range(B):
            t = ahead(k)
            push(cache_own.at[:, t], cache_out.at[:, :, cols_of(j_own)], cache_send, cache_recv, t)

    def push_hidden():
        for k in range(B):
            t = ahead(k)
            push(
                hid_own.at[pl.ds(pl.multiple_of(t * rows, rows), rows), :],
                hid_out.at[:, cols_of(j_own)], hid_send, hid_recv, t,
            )

    @pl.when(owner)
    def _():
        fresh_k = PROJ[:, hd : 2 * hd].astype(BF16)
        fresh_v = PROJ[:, 2 * hd :].astype(BF16)
        cache_own[0] = fresh_k.reshape(B, rows, hd)
        cache_own[1] = fresh_v.reshape(B, rows, hd)
        @pl.when(s == S - 1)
        def _():
            push_cache()

        with jax.named_scope("waitST"):
            arrived(ST, st_recv)
        tok_bits = tok.bit_length() - 1

        def place(shape, axis):
            at = lax.broadcasted_iota(jnp.int32, shape, axis)
            which = lax.shift_right_logical(at, tok_bits) & (micro - 1)
            spot = lax.shift_right_logical(at, rows.bit_length() - 1) * tok + (at & (tok - 1))
            return which, spot

        def per_micro(which, read):
            out = jnp.zeros(which.shape, jnp.int32)
            for m in range(micro):
                out = jnp.where(which == m, read(m), out)
            return out

        which, _ = place((total, hd), 0)
        use_stale = per_micro(which, lambda m: flags[s, m]) == 1
        kept_k = jnp.where(use_stale, ST[0].reshape(total, hd).astype(F32), fresh_k.astype(F32))
        kept_v = jnp.where(use_stale, ST[1].reshape(total, hd).astype(F32), fresh_v.astype(F32))
        keys = rms(kept_k, head_gain[1:2, :]).astype(BF16)
        queries = rms(PROJ[:, :hd], head_gain[0:1, :]).astype(BF16)
        scale = hd**-0.5
        nt = (((1,), (1,)), ((), ()))

        def attend(key_rows, value_rows, mask):
            scores = lax.dot_general(queries, key_rows, nt, preferred_element_type=F32) * scale
            probs = jnp.where(mask, jnp.exp(scores), 0.0)
            num = jnp.dot(probs.astype(BF16), value_rows, preferred_element_type=F32)
            return num, jnp.sum(probs, axis=1, keepdims=True)

        shape = (total, total)
        q_which, _ = place(shape, 0)
        k_which, k_spot = place(shape, 1)
        mask = (q_which == k_which) & (k_spot < per_micro(k_which, lambda m: patch_len[m]))
        num, den = attend(keys, kept_v.astype(BF16), mask)
        text_at = lax.broadcasted_iota(jnp.int32, (total, TK.shape[0]), 1)
        text_num, text_den = attend(TK[...], TV[...], text_at < text_len[0])
        attended = (num + text_num) / (den + text_den)
        hid_own[...] = (RES[...].reshape(total, hd).astype(F32) + attended).astype(BF16)

        @pl.when(s < S - 1)
        def _():
            for k in range(0, B, 2):
                remote(hid_own, col_block(j_own), zs.at[k // 2], zr.at[j_own], (s + 1, ahead(k), h)).start()

        @pl.when(early)
        def _():
            relay()

        @pl.when(s == S - 1)
        def _():
            push_hidden()

    @pl.when(s < S - 1)
    def _():
        with jax.named_scope("taken"):
            pl.semaphore_wait(taken, 1)

        @pl.when(owner)
        def _():
            for k in range(0, B, 2):
                sent(hid_own, zs.at[k // 2])
            push_hidden()
            push_cache()

    with jax.named_scope("waitOut"):
        arrived(hid_out, hid_recv)
        arrived(cache_out, cache_recv)

    @pl.when(owner)
    def _():
        sent(hid_own.at[pl.ds(0, total - rows), :], hid_send)
        sent(cache_own.at[:, pl.ds(0, B - 1)], cache_send)
        sent(w_in.at[:, :, pl.ds(0, width - hd)], w_send)
        sent(stale_in.at[:, :, pl.ds(0, width - hd)], st_send)

    @pl.when(jnp.logical_not(owner))
    def _():
        sent(w_in, w_send)
        sent(stale_in, st_send)

    @pl.when(early)
    def _():
        relay_done()

    @pl.when(s == 0)
    def _():
        sent(X.at[pl.ds(0, n), :, half], xm_send)
        sent(X.at[:, :, half], xc_send)

    @pl.when(s == 1)
    def _():
        sent(X.at[pl.ds(0, n - 1), :, half], x_send)

    @pl.when(s > 0)
    def _():
        sent(X1.at[h, pl.ds(0, heads // 2)], ym_send)
        sent(X1.at[h], core_send)


def store(hid, cache, hid_out, cache_out, done):
    copies = (
        pltpu.make_async_copy(hid, hid_out, done.at[0]),
        pltpu.make_async_copy(cache, cache_out, done.at[1]),
    )
    for copy in copies:
        copy.start()
    for copy in copies:
        copy.wait()


def shards(
    hidden_in, w_qkv, norm_gain, qk_gain, text_states, text_len, patch_len, stale_flags, stale_kv
):
    S, B = lax.axis_size("section"), lax.axis_size("blk")
    micro, tok, width = hidden_in.shape
    hd = qk_gain.shape[2]
    heads = width // hd
    rows = micro * tok
    total = B * rows
    depth = w_qkv.shape[1]
    text = text_states.shape[1]
    n, slots = B // 2, (heads + 1) // 2
    w = w_qkv[0].transpose(1, 0, 2)
    hbm = pl.BlockSpec(memory_space=pltpu.HBM)
    sem = pltpu.SemaphoreType.DMA
    hid, cache = pl.pallas_call(
        functools.partial(kernel, (S, B, heads, hd, micro, tok)),
        out_shape=(
            pltpu.VMEM((rows, width), BF16),
            pltpu.VMEM((2, rows, width), BF16),
        ),
        in_specs=[hbm] * 9,
        out_specs=(pl.BlockSpec(memory_space=pl.ANY),) * 2,
        scratch_shapes=[
            pltpu.SMEM(text_len.shape, jnp.int32),
            pltpu.SMEM(patch_len.shape, jnp.int32),
            pltpu.SMEM(stale_flags.shape[::-1], jnp.int32),
            pltpu.VMEM(norm_gain.shape, F32),
            pltpu.VMEM(qk_gain.shape[1:], F32),
            pltpu.VMEM((B, rows, 2 * width), BF16),
            pltpu.VMEM((2, heads, total, hd), BF16),
            pltpu.VMEM((B, rows, hd), BF16),
            pltpu.VMEM((total, 2 * width), BF16),
            pltpu.VMEM((text, 2 * width), BF16),
            pltpu.VMEM((text, 2 * width), BF16),
            pltpu.VMEM((3, B * depth, hd), BF16),
            pltpu.VMEM((slots, 3, depth, hd), BF16),
            pltpu.VMEM((total, 3 * hd), F32),
            pltpu.VMEM((2, B, rows, hd), BF16),
            pltpu.VMEM((text, hd), BF16),
            pltpu.VMEM((text, hd), BF16),
            pltpu.VMEM((total, hd), BF16),
            pltpu.VMEM((2, B, rows, hd), BF16),
            pltpu.SemaphoreType.REGULAR, pltpu.SemaphoreType.REGULAR, pltpu.SemaphoreType.REGULAR,
            sem((5,)), sem((B,)), sem((n,)), sem((heads,)), sem((heads,)),
            sem((slots,)), sem((slots,)), sem((17,)),
        ],
        compiler_params=pltpu.CompilerParams(
            collective_id=0, has_side_effects=True, vmem_limit_bytes=60 * 1024 * 1024
        ),
    )(
        text_len, patch_len, stale_flags.T,
        hidden_in.reshape(rows, width), w, norm_gain, qk_gain[0], text_states[0],
        stale_kv[0].reshape(2, rows, width),
    )
    hid, cache = pl.pallas_call(
        store,
        out_shape=(
            jax.ShapeDtypeStruct(hid.shape, BF16),
            jax.ShapeDtypeStruct(cache.shape, BF16),
        ),
        in_specs=[pl.BlockSpec(memory_space=pl.ANY)] * 2,
        out_specs=(pl.BlockSpec(memory_space=pl.ANY),) * 2,
        scratch_shapes=[sem((2,))],
    )(pltpu.with_memory_space_constraint(hid, pltpu.VMEM), pltpu.with_memory_space_constraint(cache, pltpu.VMEM))
    return (
        hid.reshape(1, micro, tok, width),
        cache.reshape(1, 2, micro, tok, width),
    )


def solution(mesh):
    in_specs = (
        P(None, "blk", "head"),
        P("section", "blk", None, "head"),
        P("section", None),
        P("section", None, None),
        P("section", None, None),
        P(),
        P(),
        P(),
        P("section", None, None, "blk", "head"),
    )
    out_specs = (P("section", None, "blk", "head"), P("section", None, None, "blk", "head"))
    return jax.shard_map(shards, mesh=mesh, in_specs=in_specs, out_specs=out_specs, check_vma=False)
```

```python
import functools

import jax
import jax.numpy as jnp
from jax import lax
from jax.experimental import pallas as pl
from jax.experimental.pallas import tpu as pltpu
from jax.sharding import PartitionSpec as P

MESH = pl.DeviceIdType.MESH
F32 = jnp.float32
BF16 = jnp.bfloat16


def rms(values, gain):
    return values * lax.rsqrt(jnp.mean(values * values, axis=-1, keepdims=True) + 1e-06) * gain


def kernel(
    dims,
    text_len_in, patch_len_in, flags_in,
    hid_in, w_in, row_gain_in, head_gain_in, text_hbm, stale_in,
    hid_out, cache_out,
    text_len, patch_len, flags, row_gain, head_gain,
    X, X1, RES, XN, text_in, TN, W, R, PROJ, ST, TK, TV,
    hid_own, cache_own,
    all_in, taken, ls, xr, zs, zr, yr, rr, fs, one,
):
    S, B, heads, hd, micro, tok = dims
    n = B // 2
    slots = (heads + 1) // 2
    rows = micro * tok
    total = B * rows
    width = heads * hd
    depth = w_in.shape[1]
    s, b, h = lax.axis_index("section"), lax.axis_index("blk"), lax.axis_index("head")
    first_owner = (B - heads) // 2
    off = first_owner - 1 + 2 * h if B - heads >= 2 else first_owner
    late = lax.rem(s, 2)
    early = late == 0
    pair = s + 1 - 2 * late
    mate = b + 1 - 2 * lax.rem(b, 2)
    my_half = b // n
    across = lax.rem(b + n, B)
    inner = lax.rem(b, n) // (n // 2) != my_half
    outer = jnp.logical_not(inner)
    j_own = b - off
    owner = (b >= off) & (b < off + heads)
    core = (s, b, 1 - h)
    half = pl.ds(pl.multiple_of(h * width, hd), width)
    other_half = pl.ds(pl.multiple_of((1 - h) * width, hd), width)
    (
        w_send, w_recv, st_send, st_recv, x_send, xm_send, xc_send, xc_recv, x_own, text_recv,
        ym_send, core_send, core_recv, hid_send, hid_recv, cache_send, cache_recv,
    ) = [one.at[i] for i in range(17)]

    def ahead(k):
        return lax.rem(b + k, B)

    def in_half(k):
        return my_half * n + lax.rem(b - my_half * n + k, n)

    def nearest(k):
        return in_half(k) if k < n else k + my_half * (2 * n - 2 - 2 * k) + lax.rem(b, 2)

    def owns(c):
        return (c >= off) & (c < off + heads)

    def near(c):
        return (c // n == my_half) | (c == across)

    def far(c):
        return jnp.logical_not(near(c))

    def remote(src, dst, send, recv, dev):
        return pltpu.make_async_remote_copy(
            src_ref=src, dst_ref=dst, send_sem=send, recv_sem=recv, device_id=dev, device_id_type=MESH
        )

    def arrived(dst, sem):
        pltpu.make_async_copy(dst, dst, sem).wait()

    def sent(src, sem):
        remote(src, src, sem, sem, core).wait_send()

    def push(src, dst, send, recv, target):
        @pl.when(target == b)
        def _():
            pltpu.make_async_copy(src, dst, recv).start()

        @pl.when(target != b)
        def _():
            remote(src, dst, send, recv, (s, target, h)).start()

    def cols_of(j):
        return pl.ds(pl.multiple_of(j * hd, hd), hd)

    def w_cols(j):
        return w_in.at[:, :, cols_of(j)]

    def w_rows(c):
        return W.at[:, pl.ds(pl.multiple_of(c * depth, depth), depth), :]

    def row_block(c):
        return X.at[c, :, half]

    barrier = pltpu.get_barrier_semaphore()

    def hello(*dev):
        pl.semaphore_signal(barrier, inc=1, device_id=dev, device_id_type=MESH)

    for k in range(n):
        hello(pair, in_half(k), h)
    for k in range(1, n):
        hello(s, in_half(k), h)
    hello(*core)
    hello(pair, across, h)
    hello(s, across, h)
    beside = jnp.where(late == 1, s + 1, s - 1)
    linked = (beside >= 0) & (beside < S)
    if S > 2:
        @pl.when(linked)
        def _():
            for k in range(0, B, 2):
                hello(beside, ahead(k), h)

    text_copy = pltpu.make_async_copy(text_hbm, text_in, text_recv)
    text_copy.start()
    small = (
        (text_len_in, text_len), (patch_len_in, patch_len), (flags_in, flags),
        (row_gain_in, row_gain), (head_gain_in, head_gain),
    )
    loads = [pltpu.make_async_copy(src, dst, ls.at[i]) for i, (src, dst) in enumerate(small)]
    for load in loads:
        load.start()

    @pl.when(s == 0)
    def _():
        pltpu.make_async_copy(hid_in, row_block(b), x_own).start()

    for load in loads:
        load.wait()
    text_copy.wait()
    TN[...] = rms(text_in[...].astype(F32), row_gain[...]).astype(BF16)

    with jax.named_scope("barrier"):
        pl.semaphore_wait(barrier, 2 * n + 2 + (linked.astype(jnp.int32) * n if S > 2 else 0))

    pl.semaphore_signal(all_in, inc=1, device_id=(s, across, h), device_id_type=MESH)

    def other_side(c, t):
        return 2 * t + lax.rem(c + off + 1, 2)

    def central(c):
        return lax.rem(c, n) // (n // 2) != c // n

    def crosses(c, j):
        return (j < heads) & ((j + off) // n != c // n)

    def detours(c, j):
        return crosses(c, j) & (lax.rem(j + off + c, 2) == 1)

    def send_relayed():
        for t in range(slots):
            j = other_side(b, t)

            @pl.when(detours(b, j))
            def _():
                remote(w_cols(j), R.at[t], w_send, rr.at[t], (pair, jnp.where(late == 1, b, mate), h)).start()

    def send_crossing(which):
        for k in range(heads):
            j = lax.rem(b + k, heads)

            @pl.when(crosses(b, j) & jnp.logical_not(detours(b, j)) & which(j + off))
            def _():
                remote(w_cols(j), w_rows(b), w_send, w_recv, (s, j + off, h)).start()

    def send_staying():
        for k in range(heads):
            j = lax.rem(b + k, heads)

            @pl.when((j + off) // n == my_half)
            def _():
                push(w_cols(j), w_rows(b), w_send, w_recv, j + off)

    def send_stale(which):
        for k in range(heads):
            j = lax.rem(b + k, heads)

            @pl.when(which(j + off))
            def _():
                push(stale_in.at[:, :, cols_of(j)], ST.at[:, b], st_send, st_recv, j + off)

    def relayed(t):
        cb = jnp.where(late == 1, mate, b)
        j = other_side(cb, t)
        return detours(cb, j), remote(R.at[t], w_rows(cb), fs.at[t], w_recv, (pair, j + off, h))

    def relay():
        for t in range(slots):
            used, onward = relayed(t)

            @pl.when(used)
            def _():
                arrived(R.at[t], rr.at[t])
                onward.start()

    def relay_done():
        for t in range(slots):
            used, _ = relayed(t)

            @pl.when(used)
            def _():
                sent(R.at[t], fs.at[t])

    def send_states(which):
        for k in range(2, B, 2):
            @pl.when(which(nearest(k)))
            def _():
                remote(hid_in, row_block(b), x_send, xr.at[b], (s - 1, nearest(k), h)).start()

    def block_to_core(c):
        return remote(row_block(c), row_block(c), xc_send, xc_recv, core)

    @pl.when(s == 1)
    def _():
        send_states(near)

    @pl.when(early)
    def _():
        send_relayed()

        @pl.when(s == 0)
        def _():
            pltpu.make_async_copy(hid_in, row_block(b), x_own).wait()
            remote(row_block(b), row_block(b), xm_send, xr.at[b], (s, mate, h)).start()
            block_to_core(b).start()

        send_stale(near)

        @pl.when(inner)
        def _():
            send_crossing(near)

    with jax.named_scope("all_in"):
        pl.semaphore_wait(all_in, 1)

    @pl.when(early)
    def _():
        send_stale(far)

        @pl.when(outer)
        def _():
            send_crossing(near)

        send_crossing(far)

        @pl.when(s == 0)
        def _():
            with jax.named_scope("xcol"):
                for k in range(2, B, 2):
                    c = nearest(k)
                    arrived(row_block(c), xr.at[c])
                    remote(row_block(c), row_block(c), xm_send, xr.at[c], (s, mate, h)).start()
                    block_to_core(c).start()

        send_staying()

    @pl.when(late == 1)
    def _():
        @pl.when(s == 1)
        def _():
            send_states(far)

        send_relayed()
        with jax.named_scope("relay"):
            relay()
        send_staying()
        with jax.named_scope("relay_done"):
            relay_done()
        send_stale(near)
        send_stale(far)
        send_crossing(near)
        send_crossing(far)

    def norm_states(values):
        XN[...] = rms(values.astype(F32), row_gain[...]).astype(BF16)

    @pl.when(s == 0)
    def _():
        with jax.named_scope("waitX"):
            for k in range(0, B, 2):
                c = nearest(k) + mate - b
                arrived(row_block(c), xr.at[c])
                block_to_core(c).start()
        with jax.named_scope("waitswap"):
            arrived(X.at[:, :, other_half], xc_recv)

        @pl.when(owner)
        def _():
            norm_states(X[...].reshape(total, 2 * width))
            RES[...] = X[:, :, pl.ds(pl.multiple_of(h * width + j_own * hd, hd), hd)]

    @pl.when(early & (jnp.logical_not(owner) | (h == 1)))
    def _():
        with jax.named_scope("relayW1"):
            relay()

    def text_part():
        @pl.when(owner)
        def _():
            with jax.named_scope("waitW"):
                arrived(W, w_recv)
            text_kv = jnp.dot(
                TN[...], jnp.concatenate([W[1], W[2]], axis=1), preferred_element_type=F32
            ).astype(BF16)
            TK[...] = rms(text_kv[:, :hd].astype(F32), head_gain[1:2, :]).astype(BF16)
            TV[...] = text_kv[:, hd:]

    @pl.when(s == 0)
    def _():
        text_part()

    def col_block(j):
        return X1.at[h, j]

    def to_core(c):
        return remote(col_block(c - off), col_block(c - off), core_send, core_recv, core)

    @pl.when(s > 0)
    def _():
        with jax.named_scope("waitX1"):
            for k in range(0, B, 2):
                c = nearest(k)

                @pl.when(owns(c))
                def _():
                    block = col_block(c - off)
                    arrived(block, zr.at[c - off])
                    remote(block, block, ym_send, yr.at[c - off], (s, mate, h)).start()
                    to_core(c).start()

        pl.semaphore_signal(taken, inc=1, device_id=(s - 1, b, h), device_id_type=MESH)
        with jax.named_scope("waitX1m"):
            for k in range(0, B, 2):
                c = nearest(k) + mate - b

                @pl.when(owns(c))
                def _():
                    arrived(col_block(c - off), yr.at[c - off])
                    to_core(c).start()

        text_part()
        with jax.named_scope("waitX1c"):
            arrived(X1.at[1 - h], core_recv)

        @pl.when(owner)
        def _():
            norm_states(jnp.concatenate([X1[i, j] for i in range(2) for j in range(heads)], axis=1))
            RES[...] = X1[h, j_own].reshape(RES.shape)

    @pl.when(owner)
    def _():
        PROJ[...] = jnp.dot(
            XN[...], jnp.concatenate([W[0], W[1], W[2]], axis=1), preferred_element_type=F32
        )

    def push_cache():
        for t in range(B):
            push(cache_own.at[:, t], cache_out.at[:, :, cols_of(j_own)], cache_send, cache_recv, t)

    def push_hidden():
        for t in range(B):
            push(
                hid_own.at[pl.ds(t * rows, rows), :],
                hid_out.at[:, cols_of(j_own)], hid_send, hid_recv, t,
            )

    @pl.when(owner)
    def _():
        fresh_k = PROJ[:, hd : 2 * hd].astype(BF16)
        fresh_v = PROJ[:, 2 * hd :].astype(BF16)
        cache_own[0] = fresh_k.reshape(B, rows, hd)
        cache_own[1] = fresh_v.reshape(B, rows, hd)
        @pl.when(s == S - 1)
        def _():
            push_cache()

        with jax.named_scope("waitST"):
            arrived(ST, st_recv)
        tok_bits = tok.bit_length() - 1

        def place(shape, axis):
            at = lax.broadcasted_iota(jnp.int32, shape, axis)
            which = lax.shift_right_logical(at, tok_bits) & (micro - 1)
            spot = lax.shift_right_logical(at, rows.bit_length() - 1) * tok + (at & (tok - 1))
            return which, spot

        def per_micro(which, read):
            out = jnp.zeros(which.shape, jnp.int32)
            for m in range(micro):
                out = jnp.where(which == m, read(m), out)
            return out

        which, _ = place((total, hd), 0)
        use_stale = per_micro(which, lambda m: flags[s, m]) == 1
        kept_k = jnp.where(use_stale, ST[0].reshape(total, hd).astype(F32), fresh_k.astype(F32))
        kept_v = jnp.where(use_stale, ST[1].reshape(total, hd).astype(F32), fresh_v.astype(F32))
        keys = rms(kept_k, head_gain[1:2, :]).astype(BF16)
        queries = rms(PROJ[:, :hd], head_gain[0:1, :]).astype(BF16)
        scale = hd**-0.5
        nt = (((1,), (1,)), ((), ()))

        def attend(key_rows, value_rows, mask):
            scores = lax.dot_general(queries, key_rows, nt, preferred_element_type=F32) * scale
            probs = jnp.where(mask, jnp.exp(scores), 0.0)
            num = jnp.dot(probs.astype(BF16), value_rows, preferred_element_type=F32)
            return num, jnp.sum(probs, axis=1, keepdims=True)

        shape = (total, total)
        q_which, _ = place(shape, 0)
        k_which, k_spot = place(shape, 1)
        mask = (q_which == k_which) & (k_spot < per_micro(k_which, lambda m: patch_len[m]))
        num, den = attend(keys, kept_v.astype(BF16), mask)
        text_at = lax.broadcasted_iota(jnp.int32, (total, TK.shape[0]), 1)
        text_num, text_den = attend(TK[...], TV[...], text_at < text_len[0])
        attended = (num + text_num) / (den + text_den)
        hid_own[...] = (RES[...].reshape(total, hd).astype(F32) + attended).astype(BF16)

        @pl.when(s < S - 1)
        def _():
            for k in range(0, B, 2):
                remote(hid_own, col_block(j_own), zs.at[k // 2], zr.at[j_own], (s + 1, ahead(k), h)).start()

        @pl.when(early & (h == 0))
        def _():
            relay()

        @pl.when(s == S - 1)
        def _():
            push_hidden()

    @pl.when(s < S - 1)
    def _():
        with jax.named_scope("taken"):
            pl.semaphore_wait(taken, 1)

        @pl.when(owner)
        def _():
            for k in range(0, B, 2):
                sent(hid_own, zs.at[k // 2])
            push_hidden()
            push_cache()

    with jax.named_scope("waitOut"):
        arrived(hid_out, hid_recv)
        arrived(cache_out, cache_recv)

    @pl.when(owner)
    def _():
        sent(hid_own.at[pl.ds(0, total - rows), :], hid_send)
        sent(cache_own.at[:, pl.ds(0, B - 1)], cache_send)
        sent(w_in.at[:, :, pl.ds(0, width - hd)], w_send)
        sent(stale_in.at[:, :, pl.ds(0, width - hd)], st_send)

    @pl.when(jnp.logical_not(owner))
    def _():
        sent(w_in, w_send)
        sent(stale_in, st_send)

    @pl.when(early)
    def _():
        relay_done()

    @pl.when(s == 0)
    def _():
        sent(X.at[pl.ds(0, n), :, half], xm_send)
        sent(X.at[:, :, half], xc_send)

    @pl.when(s == 1)
    def _():
        sent(X.at[pl.ds(0, n - 1), :, half], x_send)

    @pl.when(s > 0)
    def _():
        sent(X1.at[h, pl.ds(0, heads // 2)], ym_send)
        sent(X1.at[h], core_send)


def store(hid, cache, hid_out, cache_out, done):
    copies = (
        pltpu.make_async_copy(hid, hid_out, done.at[0]),
        pltpu.make_async_copy(cache, cache_out, done.at[1]),
    )
    for copy in copies:
        copy.start()
    for copy in copies:
        copy.wait()


def shards(
    hidden_in, w_qkv, norm_gain, qk_gain, text_states, text_len, patch_len, stale_flags, stale_kv
):
    S, B = lax.axis_size("section"), lax.axis_size("blk")
    micro, tok, width = hidden_in.shape
    hd = qk_gain.shape[2]
    heads = width // hd
    rows = micro * tok
    total = B * rows
    depth = w_qkv.shape[1]
    text = text_states.shape[1]
    n, slots = B // 2, (heads + 1) // 2
    w = w_qkv[0].transpose(1, 0, 2)
    hbm = pl.BlockSpec(memory_space=pltpu.HBM)
    sem = pltpu.SemaphoreType.DMA
    hid, cache = pl.pallas_call(
        functools.partial(kernel, (S, B, heads, hd, micro, tok)),
        out_shape=(
            pltpu.VMEM((rows, width), BF16),
            pltpu.VMEM((2, rows, width), BF16),
        ),
        in_specs=[hbm] * 9,
        out_specs=(pl.BlockSpec(memory_space=pl.ANY),) * 2,
        scratch_shapes=[
            pltpu.SMEM(text_len.shape, jnp.int32),
            pltpu.SMEM(patch_len.shape, jnp.int32),
            pltpu.SMEM(stale_flags.shape[::-1], jnp.int32),
            pltpu.VMEM(norm_gain.shape, F32),
            pltpu.VMEM(qk_gain.shape[1:], F32),
            pltpu.VMEM((B, rows, 2 * width), BF16),
            pltpu.VMEM((2, heads, total, hd), BF16),
            pltpu.VMEM((B, rows, hd), BF16),
            pltpu.VMEM((total, 2 * width), BF16),
            pltpu.VMEM((text, 2 * width), BF16),
            pltpu.VMEM((text, 2 * width), BF16),
            pltpu.VMEM((3, B * depth, hd), BF16),
            pltpu.VMEM((slots, 3, depth, hd), BF16),
            pltpu.VMEM((total, 3 * hd), F32),
            pltpu.VMEM((2, B, rows, hd), BF16),
            pltpu.VMEM((text, hd), BF16),
            pltpu.VMEM((text, hd), BF16),
            pltpu.VMEM((total, hd), BF16),
            pltpu.VMEM((2, B, rows, hd), BF16),
            pltpu.SemaphoreType.REGULAR, pltpu.SemaphoreType.REGULAR,
            sem((5,)), sem((B,)), sem((n,)), sem((heads,)), sem((heads,)),
            sem((slots,)), sem((slots,)), sem((17,)),
        ],
        compiler_params=pltpu.CompilerParams(
            collective_id=0, has_side_effects=True, vmem_limit_bytes=60 * 1024 * 1024
        ),
    )(
        text_len, patch_len, stale_flags.T,
        hidden_in.reshape(rows, width), w, norm_gain, qk_gain[0], text_states[0],
        stale_kv[0].reshape(2, rows, width),
    )
    hid, cache = pl.pallas_call(
        store,
        out_shape=(
            jax.ShapeDtypeStruct(hid.shape, BF16),
            jax.ShapeDtypeStruct(cache.shape, BF16),
        ),
        in_specs=[pl.BlockSpec(memory_space=pl.ANY)] * 2,
        out_specs=(pl.BlockSpec(memory_space=pl.ANY),) * 2,
        scratch_shapes=[sem((2,))],
    )(pltpu.with_memory_space_constraint(hid, pltpu.VMEM), pltpu.with_memory_space_constraint(cache, pltpu.VMEM))
    return (
        hid.reshape(1, micro, tok, width),
        cache.reshape(1, 2, micro, tok, width),
    )


def solution(mesh):
    in_specs = (
        P(None, "blk", "head"),
        P("section", "blk", None, "head"),
        P("section", None),
        P("section", None, None),
        P("section", None, None),
        P(),
        P(),
        P(),
        P("section", None, None, "blk", "head"),
    )
    out_specs = (P("section", None, "blk", "head"), P("section", None, None, "blk", "head"))
    return jax.shard_map(shards, mesh=mesh, in_specs=in_specs, out_specs=out_specs, check_vma=False)
```

```python
import functools

import jax
import jax.numpy as jnp
from jax import lax
from jax.experimental import pallas as pl
from jax.experimental.pallas import tpu as pltpu
from jax.sharding import PartitionSpec as P

MESH = pl.DeviceIdType.MESH
F32 = jnp.float32
BF16 = jnp.bfloat16


def rms(values, gain):
    return values * lax.rsqrt(jnp.mean(values * values, axis=-1, keepdims=True) + 1e-06) * gain


def kernel(
    dims,
    text_len_in, patch_len_in, flags_in,
    hid_in, w_in, row_gain_in, head_gain_in, text_hbm, stale_in,
    hid_out, cache_out,
    text_len, patch_len, flags, row_gain, head_gain,
    X, X1, RES, XN, text_in, TN, W, R, PROJ, ST, TK, TV,
    hid_own, cache_own,
    all_in, clear, both, taken, ls, xr, zs, zr, yr, rr, fs, one,
):
    S, B, heads, hd, micro, tok = dims
    n = B // 2
    slots = (heads + 1) // 2
    rows = micro * tok
    total = B * rows
    width = heads * hd
    depth = w_in.shape[1]
    s, b, h = lax.axis_index("section"), lax.axis_index("blk"), lax.axis_index("head")
    first_owner = (B - heads) // 2
    off = first_owner - 1 + 2 * h if B - heads >= 2 else first_owner
    late = lax.rem(s, 2)
    early = late == 0
    pair = s + 1 - 2 * late
    mate = b + 1 - 2 * lax.rem(b, 2)
    my_half = b // n
    across = lax.rem(b + n, B)
    inner = lax.rem(b, n) // (n // 2) != my_half
    outer = jnp.logical_not(inner)
    j_own = b - off
    owner = (b >= off) & (b < off + heads)
    core = (s, b, 1 - h)
    half = pl.ds(pl.multiple_of(h * width, hd), width)
    other_half = pl.ds(pl.multiple_of((1 - h) * width, hd), width)
    (
        w_send, w_recv, st_send, st_recv, x_send, xm_send, xc_send, xc_recv, x_own, text_recv,
        ym_send, core_send, core_recv, hid_send, hid_recv, cache_send, cache_recv,
    ) = [one.at[i] for i in range(17)]

    def ahead(k):
        return lax.rem(b + k, B)

    def in_half(k):
        return my_half * n + lax.rem(b - my_half * n + k, n)

    def nearest(k):
        return in_half(k) if k < n else k + my_half * (2 * n - 2 - 2 * k) + lax.rem(b, 2)

    def owns(c):
        return (c >= off) & (c < off + heads)

    def near(c):
        return (c // n == my_half) | (c == across)

    def far(c):
        return jnp.logical_not(near(c))

    def remote(src, dst, send, recv, dev):
        return pltpu.make_async_remote_copy(
            src_ref=src, dst_ref=dst, send_sem=send, recv_sem=recv, device_id=dev, device_id_type=MESH
        )

    def arrived(dst, sem):
        pltpu.make_async_copy(dst, dst, sem).wait()

    def sent(src, sem):
        remote(src, src, sem, sem, core).wait_send()

    def push(src, dst, send, recv, target):
        @pl.when(target == b)
        def _():
            pltpu.make_async_copy(src, dst, recv).start()

        @pl.when(target != b)
        def _():
            remote(src, dst, send, recv, (s, target, h)).start()

    def cols_of(j):
        return pl.ds(pl.multiple_of(j * hd, hd), hd)

    def w_cols(j):
        return w_in.at[:, :, cols_of(j)]

    def w_rows(c):
        return W.at[:, pl.ds(pl.multiple_of(c * depth, depth), depth), :]

    def row_block(c):
        return X.at[c, :, half]

    barrier = pltpu.get_barrier_semaphore()

    def hello(*dev):
        pl.semaphore_signal(barrier, inc=1, device_id=dev, device_id_type=MESH)

    for k in range(n):
        hello(pair, in_half(k), h)
    for k in range(1, n):
        hello(s, in_half(k), h)
    hello(*core)
    hello(pair, across, h)
    hello(s, across, h)
    beside = jnp.where(late == 1, s + 1, s - 1)
    linked = (beside >= 0) & (beside < S)
    if S > 2:
        @pl.when(linked)
        def _():
            for k in range(0, B, 2):
                hello(beside, ahead(k), h)

    text_copy = pltpu.make_async_copy(text_hbm, text_in, text_recv)
    text_copy.start()
    small = (
        (text_len_in, text_len), (patch_len_in, patch_len), (flags_in, flags),
        (row_gain_in, row_gain), (head_gain_in, head_gain),
    )
    loads = [pltpu.make_async_copy(src, dst, ls.at[i]) for i, (src, dst) in enumerate(small)]
    for load in loads:
        load.start()

    @pl.when(s == 0)
    def _():
        pltpu.make_async_copy(hid_in, row_block(b), x_own).start()

    for load in loads:
        load.wait()
    text_copy.wait()
    TN[...] = rms(text_in[...].astype(F32), row_gain[...]).astype(BF16)

    with jax.named_scope("barrier"):
        pl.semaphore_wait(barrier, 2 * n + 2 + (linked.astype(jnp.int32) * n if S > 2 else 0))

    pl.semaphore_signal(all_in, inc=1, device_id=(s, across, h), device_id_type=MESH)

    def other_side(c, t, role):
        return 2 * t + lax.rem(c + off + 1 + role, 2)

    def crosses(c, j):
        return (j < heads) & ((j + off) // n != c // n)

    def detours(c, j, role):
        return crosses(c, j) & (lax.rem(j + off + c + role, 2) == 1)

    def send_relayed():
        for t in range(slots):
            j = other_side(b, t, late)

            @pl.when(detours(b, j, late))
            def _():
                remote(w_cols(j), R.at[t], w_send, rr.at[t], (pair, jnp.where(late == 1, b, mate), h)).start()

    def send_crossing(which):
        for k in range(heads):
            j = lax.rem(b + k, heads)

            @pl.when(crosses(b, j) & jnp.logical_not(detours(b, j, late)) & which(j + off))
            def _():
                remote(w_cols(j), w_rows(b), w_send, w_recv, (s, j + off, h)).start()

    def send_staying():
        for k in range(heads):
            j = lax.rem(b + k, heads)

            @pl.when((j + off) // n == my_half)
            def _():
                push(w_cols(j), w_rows(b), w_send, w_recv, j + off)

    def send_stale(which):
        for k in range(heads):
            j = lax.rem(b + k, heads)

            @pl.when(which(j + off))
            def _():
                push(stale_in.at[:, :, cols_of(j)], ST.at[:, b], st_send, st_recv, j + off)

    def relayed(t):
        cb = jnp.where(late == 1, mate, b)
        j = other_side(cb, t, 1 - late)
        return detours(cb, j, 1 - late), remote(R.at[t], w_rows(cb), fs.at[t], w_recv, (pair, j + off, h))

    def relay():
        for t in range(slots):
            used, onward = relayed(t)

            @pl.when(used)
            def _():
                arrived(R.at[t], rr.at[t])
                onward.start()

    def relay_done():
        for t in range(slots):
            used, _ = relayed(t)

            @pl.when(used)
            def _():
                sent(R.at[t], fs.at[t])

    def send_states(which):
        for k in range(2, B, 2):
            @pl.when(which(nearest(k)))
            def _():
                remote(hid_in, row_block(b), x_send, xr.at[b], (s - 1, nearest(k), h)).start()

    def block_to_core(c):
        return remote(row_block(c), row_block(c), xc_send, xc_recv, core)

    @pl.when(s == 1)
    def _():
        send_states(near)

    @pl.when(early)
    def _():
        send_relayed()

        @pl.when(s == 0)
        def _():
            pltpu.make_async_copy(hid_in, row_block(b), x_own).wait()
            remote(row_block(b), row_block(b), xm_send, xr.at[b], (s, mate, h)).start()
            block_to_core(b).start()

        send_stale(near)

        @pl.when(inner)
        def _():
            send_crossing(near)

    with jax.named_scope("all_in"):
        pl.semaphore_wait(all_in, 1)

    @pl.when(early)
    def _():
        send_stale(far)

        @pl.when(outer)
        def _():
            send_crossing(near)

        send_crossing(far)

        @pl.when(s == 0)
        def _():
            with jax.named_scope("xcol"):
                for k in range(2, B, 2):
                    c = nearest(k)
                    arrived(row_block(c), xr.at[c])
                    remote(row_block(c), row_block(c), xm_send, xr.at[c], (s, mate, h)).start()
                    block_to_core(c).start()

        send_staying()

    @pl.when(late == 1)
    def _():
        @pl.when(s == 1)
        def _():
            send_states(far)

        send_relayed()
        with jax.named_scope("relay"):
            relay()
        send_staying()
        with jax.named_scope("relay_done"):
            relay_done()
        for k in range(2, n, 2):
            pl.semaphore_signal(clear, inc=1, device_id=(s, in_half(k), h), device_id_type=MESH)
        with jax.named_scope("clear"):
            pl.semaphore_wait(clear, n // 2 - 1)
        pl.semaphore_signal(both, inc=1, device_id=core, device_id_type=MESH)
        with jax.named_scope("both"):
            pl.semaphore_wait(both, 1)
        send_crossing(far)
        send_crossing(near)
        send_stale(near)
        send_stale(far)

    def norm_states(values):
        XN[...] = rms(values.astype(F32), row_gain[...]).astype(BF16)

    @pl.when(s == 0)
    def _():
        with jax.named_scope("waitX"):
            for k in range(0, B, 2):
                c = nearest(k) + mate - b
                arrived(row_block(c), xr.at[c])
                block_to_core(c).start()
        with jax.named_scope("waitswap"):
            arrived(X.at[:, :, other_half], xc_recv)

        @pl.when(owner)
        def _():
            norm_states(X[...].reshape(total, 2 * width))
            RES[...] = X[:, :, pl.ds(pl.multiple_of(h * width + j_own * hd, hd), hd)]

    @pl.when(early & jnp.logical_not(owner))
    def _():
        with jax.named_scope("relayW1"):
            relay()

    def text_part():
        @pl.when(owner)
        def _():
            with jax.named_scope("waitW"):
                arrived(W, w_recv)
            text_kv = jnp.dot(
                TN[...], jnp.concatenate([W[1], W[2]], axis=1), preferred_element_type=F32
            ).astype(BF16)
            TK[...] = rms(text_kv[:, :hd].astype(F32), head_gain[1:2, :]).astype(BF16)
            TV[...] = text_kv[:, hd:]

    @pl.when(s == 0)
    def _():
        text_part()

    def col_block(j):
        return X1.at[h, j]

    def to_core(c):
        return remote(col_block(c - off), col_block(c - off), core_send, core_recv, core)

    @pl.when(s > 0)
    def _():
        with jax.named_scope("waitX1"):
            for k in range(0, B, 2):
                c = nearest(k)

                @pl.when(owns(c))
                def _():
                    block = col_block(c - off)
                    arrived(block, zr.at[c - off])
                    remote(block, block, ym_send, yr.at[c - off], (s, mate, h)).start()
                    to_core(c).start()

        pl.semaphore_signal(taken, inc=1, device_id=(s - 1, b, h), device_id_type=MESH)
        with jax.named_scope("waitX1m"):
            for k in range(0, B, 2):
                c = nearest(k) + mate - b

                @pl.when(owns(c))
                def _():
                    arrived(col_block(c - off), yr.at[c - off])
                    to_core(c).start()

        text_part()
        with jax.named_scope("waitX1c"):
            arrived(X1.at[1 - h], core_recv)

        @pl.when(owner)
        def _():
            norm_states(jnp.concatenate([X1[i, j] for i in range(2) for j in range(heads)], axis=1))
            RES[...] = X1[h, j_own].reshape(RES.shape)

    @pl.when(owner)
    def _():
        PROJ[...] = jnp.dot(
            XN[...], jnp.concatenate([W[0], W[1], W[2]], axis=1), preferred_element_type=F32
        )

    def push_cache():
        for t in range(B):
            push(cache_own.at[:, t], cache_out.at[:, :, cols_of(j_own)], cache_send, cache_recv, t)

    def push_hidden():
        for t in range(B):
            push(
                hid_own.at[pl.ds(t * rows, rows), :],
                hid_out.at[:, cols_of(j_own)], hid_send, hid_recv, t,
            )

    @pl.when(owner)
    def _():
        fresh_k = PROJ[:, hd : 2 * hd].astype(BF16)
        fresh_v = PROJ[:, 2 * hd :].astype(BF16)
        cache_own[0] = fresh_k.reshape(B, rows, hd)
        cache_own[1] = fresh_v.reshape(B, rows, hd)
        @pl.when(s == S - 1)
        def _():
            push_cache()

        with jax.named_scope("waitST"):
            arrived(ST, st_recv)
        tok_bits = tok.bit_length() - 1

        def place(shape, axis):
            at = lax.broadcasted_iota(jnp.int32, shape, axis)
            which = lax.shift_right_logical(at, tok_bits) & (micro - 1)
            spot = lax.shift_right_logical(at, rows.bit_length() - 1) * tok + (at & (tok - 1))
            return which, spot

        def per_micro(which, read):
            out = jnp.zeros(which.shape, jnp.int32)
            for m in range(micro):
                out = jnp.where(which == m, read(m), out)
            return out

        which, _ = place((total, hd), 0)
        use_stale = per_micro(which, lambda m: flags[s, m]) == 1
        kept_k = jnp.where(use_stale, ST[0].reshape(total, hd).astype(F32), fresh_k.astype(F32))
        kept_v = jnp.where(use_stale, ST[1].reshape(total, hd).astype(F32), fresh_v.astype(F32))
        keys = rms(kept_k, head_gain[1:2, :]).astype(BF16)
        queries = rms(PROJ[:, :hd], head_gain[0:1, :]).astype(BF16)
        scale = hd**-0.5
        nt = (((1,), (1,)), ((), ()))

        def attend(key_rows, value_rows, mask):
            scores = lax.dot_general(queries, key_rows, nt, preferred_element_type=F32) * scale
            probs = jnp.where(mask, jnp.exp(scores), 0.0)
            num = jnp.dot(probs.astype(BF16), value_rows, preferred_element_type=F32)
            return num, jnp.sum(probs, axis=1, keepdims=True)

        shape = (total, total)
        q_which, _ = place(shape, 0)
        k_which, k_spot = place(shape, 1)
        mask = (q_which == k_which) & (k_spot < per_micro(k_which, lambda m: patch_len[m]))
        num, den = attend(keys, kept_v.astype(BF16), mask)
        text_at = lax.broadcasted_iota(jnp.int32, (total, TK.shape[0]), 1)
        text_num, text_den = attend(TK[...], TV[...], text_at < text_len[0])
        attended = (num + text_num) / (den + text_den)
        hid_own[...] = (RES[...].reshape(total, hd).astype(F32) + attended).astype(BF16)

        @pl.when(s < S - 1)
        def _():
            for k in range(0, B, 2):
                remote(hid_own, col_block(j_own), zs.at[k // 2], zr.at[j_own], (s + 1, ahead(k), h)).start()

        @pl.when(early)
        def _():
            relay()

        @pl.when(s == S - 1)
        def _():
            push_hidden()

    @pl.when(s < S - 1)
    def _():
        with jax.named_scope("taken"):
            pl.semaphore_wait(taken, 1)

        @pl.when(owner)
        def _():
            for k in range(0, B, 2):
                sent(hid_own, zs.at[k // 2])
            push_hidden()
            push_cache()

    with jax.named_scope("waitOut"):
        arrived(hid_out, hid_recv)
        arrived(cache_out, cache_recv)

    @pl.when(owner)
    def _():
        sent(hid_own.at[pl.ds(0, total - rows), :], hid_send)
        sent(cache_own.at[:, pl.ds(0, B - 1)], cache_send)
        sent(w_in.at[:, :, pl.ds(0, width - hd)], w_send)
        sent(stale_in.at[:, :, pl.ds(0, width - hd)], st_send)

    @pl.when(jnp.logical_not(owner))
    def _():
        sent(w_in, w_send)
        sent(stale_in, st_send)

    @pl.when(early)
    def _():
        relay_done()

    @pl.when(s == 0)
    def _():
        sent(X.at[pl.ds(0, n), :, half], xm_send)
        sent(X.at[:, :, half], xc_send)

    @pl.when(s == 1)
    def _():
        sent(X.at[pl.ds(0, n - 1), :, half], x_send)

    @pl.when(s > 0)
    def _():
        sent(X1.at[h, pl.ds(0, heads // 2)], ym_send)
        sent(X1.at[h], core_send)


def store(hid, cache, hid_out, cache_out, done):
    copies = (
        pltpu.make_async_copy(hid, hid_out, done.at[0]),
        pltpu.make_async_copy(cache, cache_out, done.at[1]),
    )
    for copy in copies:
        copy.start()
    for copy in copies:
        copy.wait()


def shards(
    hidden_in, w_qkv, norm_gain, qk_gain, text_states, text_len, patch_len, stale_flags, stale_kv
):
    S, B = lax.axis_size("section"), lax.axis_size("blk")
    micro, tok, width = hidden_in.shape
    hd = qk_gain.shape[2]
    heads = width // hd
    rows = micro * tok
    total = B * rows
    depth = w_qkv.shape[1]
    text = text_states.shape[1]
    n, slots = B // 2, (heads + 1) // 2
    w = w_qkv[0].transpose(1, 0, 2)
    hbm = pl.BlockSpec(memory_space=pltpu.HBM)
    sem = pltpu.SemaphoreType.DMA
    hid, cache = pl.pallas_call(
        functools.partial(kernel, (S, B, heads, hd, micro, tok)),
        out_shape=(
            pltpu.VMEM((rows, width), BF16),
            pltpu.VMEM((2, rows, width), BF16),
        ),
        in_specs=[hbm] * 9,
        out_specs=(pl.BlockSpec(memory_space=pl.ANY),) * 2,
        scratch_shapes=[
            pltpu.SMEM(text_len.shape, jnp.int32),
            pltpu.SMEM(patch_len.shape, jnp.int32),
            pltpu.SMEM(stale_flags.shape[::-1], jnp.int32),
            pltpu.VMEM(norm_gain.shape, F32),
            pltpu.VMEM(qk_gain.shape[1:], F32),
            pltpu.VMEM((B, rows, 2 * width), BF16),
            pltpu.VMEM((2, heads, total, hd), BF16),
            pltpu.VMEM((B, rows, hd), BF16),
            pltpu.VMEM((total, 2 * width), BF16),
            pltpu.VMEM((text, 2 * width), BF16),
            pltpu.VMEM((text, 2 * width), BF16),
            pltpu.VMEM((3, B * depth, hd), BF16),
            pltpu.VMEM((slots, 3, depth, hd), BF16),
            pltpu.VMEM((total, 3 * hd), F32),
            pltpu.VMEM((2, B, rows, hd), BF16),
            pltpu.VMEM((text, hd), BF16),
            pltpu.VMEM((text, hd), BF16),
            pltpu.VMEM((total, hd), BF16),
            pltpu.VMEM((2, B, rows, hd), BF16),
            pltpu.SemaphoreType.REGULAR, pltpu.SemaphoreType.REGULAR,
            pltpu.SemaphoreType.REGULAR, pltpu.SemaphoreType.REGULAR,
            sem((5,)), sem((B,)), sem((n,)), sem((heads,)), sem((heads,)),
            sem((slots,)), sem((slots,)), sem((17,)),
        ],
        compiler_params=pltpu.CompilerParams(
            collective_id=0, has_side_effects=True, vmem_limit_bytes=60 * 1024 * 1024
        ),
    )(
        text_len, patch_len, stale_flags.T,
        hidden_in.reshape(rows, width), w, norm_gain, qk_gain[0], text_states[0],
        stale_kv[0].reshape(2, rows, width),
    )
    hid, cache = pl.pallas_call(
        store,
        out_shape=(
            jax.ShapeDtypeStruct(hid.shape, BF16),
            jax.ShapeDtypeStruct(cache.shape, BF16),
        ),
        in_specs=[pl.BlockSpec(memory_space=pl.ANY)] * 2,
        out_specs=(pl.BlockSpec(memory_space=pl.ANY),) * 2,
        scratch_shapes=[sem((2,))],
    )(pltpu.with_memory_space_constraint(hid, pltpu.VMEM), pltpu.with_memory_space_constraint(cache, pltpu.VMEM))
    return (
        hid.reshape(1, micro, tok, width),
        cache.reshape(1, 2, micro, tok, width),
    )


def solution(mesh):
    in_specs = (
        P(None, "blk", "head"),
        P("section", "blk", None, "head"),
        P("section", None),
        P("section", None, None),
        P("section", None, None),
        P(),
        P(),
        P(),
        P("section", None, None, "blk", "head"),
    )
    out_specs = (P("section", None, "blk", "head"), P("section", None, None, "blk", "head"))
    return jax.shard_map(shards, mesh=mesh, in_specs=in_specs, out_specs=out_specs, check_vma=False)
```

```python
import functools

import jax
import jax.numpy as jnp
from jax import lax
from jax.experimental import pallas as pl
from jax.experimental.pallas import tpu as pltpu
from jax.sharding import PartitionSpec as P

MESH = pl.DeviceIdType.MESH
F32 = jnp.float32
BF16 = jnp.bfloat16


def rms(values, gain):
    return values * lax.rsqrt(jnp.mean(values * values, axis=-1, keepdims=True) + 1e-06) * gain


def kernel(
    dims,
    text_len_in, patch_len_in, flags_in,
    hid_in, w_in, row_gain_in, head_gain_in, text_hbm, stale_in,
    hid_out, cache_out,
    text_len, patch_len, flags, row_gain, head_gain,
    X, X1, RES, XN, text_in, TN, W, R, PROJ, ST, TK, TV,
    hid_own, cache_own,
    all_in, clear, both, taken, ls, xr, zs, zr, yr, rr, fs, one,
):
    S, B, heads, hd, micro, tok = dims
    n = B // 2
    slots = (heads + 1) // 2
    rows = micro * tok
    total = B * rows
    width = heads * hd
    depth = w_in.shape[1]
    s, b, h = lax.axis_index("section"), lax.axis_index("blk"), lax.axis_index("head")
    first_owner = (B - heads) // 2
    off = first_owner - 1 + 2 * h if B - heads >= 2 else first_owner
    late = lax.rem(s, 2)
    early = late == 0
    pair = s + 1 - 2 * late
    mate = b + 1 - 2 * lax.rem(b, 2)
    my_half = b // n
    across = lax.rem(b + n, B)
    inner = lax.rem(b, n) // (n // 2) != my_half
    outer = jnp.logical_not(inner)
    j_own = b - off
    owner = (b >= off) & (b < off + heads)
    core = (s, b, 1 - h)
    half = pl.ds(pl.multiple_of(h * width, hd), width)
    other_half = pl.ds(pl.multiple_of((1 - h) * width, hd), width)
    (
        w_send, w_recv, st_send, st_recv, x_send, xm_send, xc_send, xc_recv, x_own, text_recv,
        ym_send, core_send, core_recv, hid_send, hid_recv, cache_send, cache_recv,
    ) = [one.at[i] for i in range(17)]

    def ahead(k):
        return lax.rem(b + k, B)

    def in_half(k):
        return my_half * n + lax.rem(b - my_half * n + k, n)

    def nearest(k):
        return in_half(k) if k < n else k + my_half * (2 * n - 2 - 2 * k) + lax.rem(b, 2)

    def owns(c):
        return (c >= off) & (c < off + heads)

    def near(c):
        return (c // n == my_half) | (c == across)

    def far(c):
        return jnp.logical_not(near(c))

    def remote(src, dst, send, recv, dev):
        return pltpu.make_async_remote_copy(
            src_ref=src, dst_ref=dst, send_sem=send, recv_sem=recv, device_id=dev, device_id_type=MESH
        )

    def arrived(dst, sem):
        pltpu.make_async_copy(dst, dst, sem).wait()

    def sent(src, sem):
        remote(src, src, sem, sem, core).wait_send()

    def push(src, dst, send, recv, target):
        @pl.when(target == b)
        def _():
            pltpu.make_async_copy(src, dst, recv).start()

        @pl.when(target != b)
        def _():
            remote(src, dst, send, recv, (s, target, h)).start()

    def cols_of(j):
        return pl.ds(pl.multiple_of(j * hd, hd), hd)

    def w_cols(j):
        return w_in.at[:, :, cols_of(j)]

    def w_rows(c):
        return W.at[:, pl.ds(pl.multiple_of(c * depth, depth), depth), :]

    def row_block(c):
        return X.at[c, :, half]

    barrier = pltpu.get_barrier_semaphore()

    def hello(*dev):
        pl.semaphore_signal(barrier, inc=1, device_id=dev, device_id_type=MESH)

    for k in range(n):
        hello(pair, in_half(k), h)
    for k in range(1, n):
        hello(s, in_half(k), h)
    hello(*core)
    hello(pair, across, h)
    hello(s, across, h)
    beside = jnp.where(late == 1, s + 1, s - 1)
    linked = (beside >= 0) & (beside < S)
    if S > 2:
        @pl.when(linked)
        def _():
            for k in range(0, B, 2):
                hello(beside, ahead(k), h)

    text_copy = pltpu.make_async_copy(text_hbm, text_in, text_recv)
    text_copy.start()
    small = (
        (text_len_in, text_len), (patch_len_in, patch_len), (flags_in, flags),
        (row_gain_in, row_gain), (head_gain_in, head_gain),
    )
    loads = [pltpu.make_async_copy(src, dst, ls.at[i]) for i, (src, dst) in enumerate(small)]
    for load in loads:
        load.start()

    @pl.when(s == 0)
    def _():
        pltpu.make_async_copy(hid_in, row_block(b), x_own).start()


    with jax.named_scope("barrier"):
        pl.semaphore_wait(barrier, 2 * n + 2 + (linked.astype(jnp.int32) * n if S > 2 else 0))

    pl.semaphore_signal(all_in, inc=1, device_id=(s, across, h), device_id_type=MESH)

    def other_side(c, t, role):
        return 2 * t + lax.rem(c + off + 1 + role, 2)

    def crosses(c, j):
        return (j < heads) & ((j + off) // n != c // n)

    def detours(c, j, role):
        return crosses(c, j) & (lax.rem(j + off + c + role, 2) == 1)

    def send_relayed():
        for t in range(slots):
            j = other_side(b, t, late)

            @pl.when(detours(b, j, late))
            def _():
                remote(w_cols(j), R.at[t], w_send, rr.at[t], (pair, jnp.where(late == 1, b, mate), h)).start()

    def send_crossing(which):
        for k in range(heads):
            j = lax.rem(b + k, heads)

            @pl.when(crosses(b, j) & jnp.logical_not(detours(b, j, late)) & which(j + off))
            def _():
                remote(w_cols(j), w_rows(b), w_send, w_recv, (s, j + off, h)).start()

    def send_staying():
        for k in range(heads):
            j = lax.rem(b + k, heads)

            @pl.when((j + off) // n == my_half)
            def _():
                push(w_cols(j), w_rows(b), w_send, w_recv, j + off)

    def send_stale(which):
        for k in range(heads):
            j = lax.rem(b + k, heads)

            @pl.when(which(j + off))
            def _():
                push(stale_in.at[:, :, cols_of(j)], ST.at[:, b], st_send, st_recv, j + off)

    def relayed(t):
        cb = jnp.where(late == 1, mate, b)
        j = other_side(cb, t, 1 - late)
        return detours(cb, j, 1 - late), remote(R.at[t], w_rows(cb), fs.at[t], w_recv, (pair, j + off, h))

    def relay():
        for t in range(slots):
            used, onward = relayed(t)

            @pl.when(used)
            def _():
                arrived(R.at[t], rr.at[t])
                onward.start()

    def relay_done():
        for t in range(slots):
            used, _ = relayed(t)

            @pl.when(used)
            def _():
                sent(R.at[t], fs.at[t])

    def send_states(which):
        for k in range(2, B, 2):
            @pl.when(which(nearest(k)))
            def _():
                remote(hid_in, row_block(b), x_send, xr.at[b], (s - 1, nearest(k), h)).start()

    def block_to_core(c):
        return remote(row_block(c), row_block(c), xc_send, xc_recv, core)

    @pl.when(s == 1)
    def _():
        send_states(near)

    @pl.when(early)
    def _():
        send_relayed()

        @pl.when(s == 0)
        def _():
            pltpu.make_async_copy(hid_in, row_block(b), x_own).wait()
            remote(row_block(b), row_block(b), xm_send, xr.at[b], (s, mate, h)).start()
            block_to_core(b).start()

        send_stale(near)

        @pl.when(inner)
        def _():
            send_crossing(near)

    for load in loads:
        load.wait()
    text_copy.wait()
    TN[...] = rms(text_in[...].astype(F32), row_gain[...]).astype(BF16)
    with jax.named_scope("all_in"):
        pl.semaphore_wait(all_in, 1)

    @pl.when(early)
    def _():
        send_stale(far)

        @pl.when(outer)
        def _():
            send_crossing(near)

        send_crossing(far)

        @pl.when(s == 0)
        def _():
            with jax.named_scope("xcol"):
                for k in range(2, B, 2):
                    c = nearest(k)
                    arrived(row_block(c), xr.at[c])
                    remote(row_block(c), row_block(c), xm_send, xr.at[c], (s, mate, h)).start()
                    block_to_core(c).start()

        send_staying()

    @pl.when(late == 1)
    def _():
        @pl.when(s == 1)
        def _():
            send_states(far)

        send_relayed()
        with jax.named_scope("relay"):
            relay()
        send_staying()
        with jax.named_scope("relay_done"):
            relay_done()
        for k in range(2, n, 2):
            pl.semaphore_signal(clear, inc=1, device_id=(s, in_half(k), h), device_id_type=MESH)
        with jax.named_scope("clear"):
            pl.semaphore_wait(clear, n // 2 - 1)
        pl.semaphore_signal(both, inc=1, device_id=core, device_id_type=MESH)
        with jax.named_scope("both"):
            pl.semaphore_wait(both, 1)
        send_crossing(far)
        send_crossing(near)
        send_stale(near)
        send_stale(far)

    def norm_states(values):
        XN[...] = rms(values.astype(F32), row_gain[...]).astype(BF16)

    @pl.when(s == 0)
    def _():
        with jax.named_scope("waitX"):
            for k in range(0, B, 2):
                c = nearest(k) + mate - b
                arrived(row_block(c), xr.at[c])
                block_to_core(c).start()
        with jax.named_scope("waitswap"):
            arrived(X.at[:, :, other_half], xc_recv)

        @pl.when(owner)
        def _():
            norm_states(X[...].reshape(total, 2 * width))
            RES[...] = X[:, :, pl.ds(pl.multiple_of(h * width + j_own * hd, hd), hd)]

    @pl.when(early & jnp.logical_not(owner))
    def _():
        with jax.named_scope("relayW1"):
            relay()

    def text_part():
        @pl.when(owner)
        def _():
            with jax.named_scope("waitW"):
                arrived(W, w_recv)
            text_kv = jnp.dot(
                TN[...], jnp.concatenate([W[1], W[2]], axis=1), preferred_element_type=F32
            ).astype(BF16)
            TK[...] = rms(text_kv[:, :hd].astype(F32), head_gain[1:2, :]).astype(BF16)
            TV[...] = text_kv[:, hd:]

    @pl.when(s == 0)
    def _():
        text_part()

    def col_block(j):
        return X1.at[h, j]

    def to_core(c):
        return remote(col_block(c - off), col_block(c - off), core_send, core_recv, core)

    @pl.when(s > 0)
    def _():
        with jax.named_scope("waitX1"):
            for k in range(0, B, 2):
                c = nearest(k)

                @pl.when(owns(c))
                def _():
                    block = col_block(c - off)
                    arrived(block, zr.at[c - off])
                    remote(block, block, ym_send, yr.at[c - off], (s, mate, h)).start()
                    to_core(c).start()

        pl.semaphore_signal(taken, inc=1, device_id=(s - 1, b, h), device_id_type=MESH)
        with jax.named_scope("waitX1m"):
            for k in range(0, B, 2):
                c = nearest(k) + mate - b

                @pl.when(owns(c))
                def _():
                    arrived(col_block(c - off), yr.at[c - off])
                    to_core(c).start()

        text_part()
        with jax.named_scope("waitX1c"):
            arrived(X1.at[1 - h], core_recv)

        @pl.when(owner)
        def _():
            norm_states(jnp.concatenate([X1[i, j] for i in range(2) for j in range(heads)], axis=1))
            RES[...] = X1[h, j_own].reshape(RES.shape)

    @pl.when(owner)
    def _():
        PROJ[...] = jnp.dot(
            XN[...], jnp.concatenate([W[0], W[1], W[2]], axis=1), preferred_element_type=F32
        )

    def push_cache():
        for t in range(B):
            push(cache_own.at[:, t], cache_out.at[:, :, cols_of(j_own)], cache_send, cache_recv, t)

    def push_hidden():
        for t in range(B):
            push(
                hid_own.at[pl.ds(t * rows, rows), :],
                hid_out.at[:, cols_of(j_own)], hid_send, hid_recv, t,
            )

    @pl.when(owner)
    def _():
        fresh_k = PROJ[:, hd : 2 * hd].astype(BF16)
        fresh_v = PROJ[:, 2 * hd :].astype(BF16)
        cache_own[0] = fresh_k.reshape(B, rows, hd)
        cache_own[1] = fresh_v.reshape(B, rows, hd)
        @pl.when(s == S - 1)
        def _():
            push_cache()

        with jax.named_scope("waitST"):
            arrived(ST, st_recv)
        tok_bits = tok.bit_length() - 1

        def place(shape, axis):
            at = lax.broadcasted_iota(jnp.int32, shape, axis)
            which = lax.shift_right_logical(at, tok_bits) & (micro - 1)
            spot = lax.shift_right_logical(at, rows.bit_length() - 1) * tok + (at & (tok - 1))
            return which, spot

        def per_micro(which, read):
            out = jnp.zeros(which.shape, jnp.int32)
            for m in range(micro):
                out = jnp.where(which == m, read(m), out)
            return out

        which, _ = place((total, hd), 0)
        use_stale = per_micro(which, lambda m: flags[s, m]) == 1
        kept_k = jnp.where(use_stale, ST[0].reshape(total, hd).astype(F32), fresh_k.astype(F32))
        kept_v = jnp.where(use_stale, ST[1].reshape(total, hd).astype(F32), fresh_v.astype(F32))
        keys = rms(kept_k, head_gain[1:2, :]).astype(BF16)
        queries = rms(PROJ[:, :hd], head_gain[0:1, :]).astype(BF16)
        scale = hd**-0.5
        nt = (((1,), (1,)), ((), ()))

        def attend(key_rows, value_rows, mask):
            scores = lax.dot_general(queries, key_rows, nt, preferred_element_type=F32) * scale
            probs = jnp.where(mask, jnp.exp(scores), 0.0)
            num = jnp.dot(probs.astype(BF16), value_rows, preferred_element_type=F32)
            return num, jnp.sum(probs, axis=1, keepdims=True)

        shape = (total, total)
        q_which, _ = place(shape, 0)
        k_which, k_spot = place(shape, 1)
        mask = (q_which == k_which) & (k_spot < per_micro(k_which, lambda m: patch_len[m]))
        num, den = attend(keys, kept_v.astype(BF16), mask)
        text_at = lax.broadcasted_iota(jnp.int32, (total, TK.shape[0]), 1)
        text_num, text_den = attend(TK[...], TV[...], text_at < text_len[0])
        attended = (num + text_num) / (den + text_den)
        hid_own[...] = (RES[...].reshape(total, hd).astype(F32) + attended).astype(BF16)

        @pl.when(s < S - 1)
        def _():
            for k in range(0, B, 2):
                remote(hid_own, col_block(j_own), zs.at[k // 2], zr.at[j_own], (s + 1, ahead(k), h)).start()

        @pl.when(early)
        def _():
            relay()

        @pl.when(s == S - 1)
        def _():
            push_hidden()

    @pl.when(s < S - 1)
    def _():
        with jax.named_scope("taken"):
            pl.semaphore_wait(taken, 1)

        @pl.when(owner)
        def _():
            for k in range(0, B, 2):
                sent(hid_own, zs.at[k // 2])
            push_hidden()
            push_cache()

    with jax.named_scope("waitOut"):
        arrived(hid_out, hid_recv)
        arrived(cache_out, cache_recv)

    @pl.when(owner)
    def _():
        sent(hid_own.at[pl.ds(0, total - rows), :], hid_send)
        sent(cache_own.at[:, pl.ds(0, B - 1)], cache_send)
        sent(w_in.at[:, :, pl.ds(0, width - hd)], w_send)
        sent(stale_in.at[:, :, pl.ds(0, width - hd)], st_send)

    @pl.when(jnp.logical_not(owner))
    def _():
        sent(w_in, w_send)
        sent(stale_in, st_send)

    @pl.when(early)
    def _():
        relay_done()

    @pl.when(s == 0)
    def _():
        sent(X.at[pl.ds(0, n), :, half], xm_send)
        sent(X.at[:, :, half], xc_send)

    @pl.when(s == 1)
    def _():
        sent(X.at[pl.ds(0, n - 1), :, half], x_send)

    @pl.when(s > 0)
    def _():
        sent(X1.at[h, pl.ds(0, heads // 2)], ym_send)
        sent(X1.at[h], core_send)


def store(hid, cache, hid_out, cache_out, done):
    copies = (
        pltpu.make_async_copy(hid, hid_out, done.at[0]),
        pltpu.make_async_copy(cache, cache_out, done.at[1]),
    )
    for copy in copies:
        copy.start()
    for copy in copies:
        copy.wait()


def shards(
    hidden_in, w_qkv, norm_gain, qk_gain, text_states, text_len, patch_len, stale_flags, stale_kv
):
    S, B = lax.axis_size("section"), lax.axis_size("blk")
    micro, tok, width = hidden_in.shape
    hd = qk_gain.shape[2]
    heads = width // hd
    rows = micro * tok
    total = B * rows
    depth = w_qkv.shape[1]
    text = text_states.shape[1]
    n, slots = B // 2, (heads + 1) // 2
    w = w_qkv[0].transpose(1, 0, 2)
    hbm = pl.BlockSpec(memory_space=pltpu.HBM)
    sem = pltpu.SemaphoreType.DMA
    hid, cache = pl.pallas_call(
        functools.partial(kernel, (S, B, heads, hd, micro, tok)),
        out_shape=(
            pltpu.VMEM((rows, width), BF16),
            pltpu.VMEM((2, rows, width), BF16),
        ),
        in_specs=[hbm] * 9,
        out_specs=(pl.BlockSpec(memory_space=pl.ANY),) * 2,
        scratch_shapes=[
            pltpu.SMEM(text_len.shape, jnp.int32),
            pltpu.SMEM(patch_len.shape, jnp.int32),
            pltpu.SMEM(stale_flags.shape[::-1], jnp.int32),
            pltpu.VMEM(norm_gain.shape, F32),
            pltpu.VMEM(qk_gain.shape[1:], F32),
            pltpu.VMEM((B, rows, 2 * width), BF16),
            pltpu.VMEM((2, heads, total, hd), BF16),
            pltpu.VMEM((B, rows, hd), BF16),
            pltpu.VMEM((total, 2 * width), BF16),
            pltpu.VMEM((text, 2 * width), BF16),
            pltpu.VMEM((text, 2 * width), BF16),
            pltpu.VMEM((3, B * depth, hd), BF16),
            pltpu.VMEM((slots, 3, depth, hd), BF16),
            pltpu.VMEM((total, 3 * hd), F32),
            pltpu.VMEM((2, B, rows, hd), BF16),
            pltpu.VMEM((text, hd), BF16),
            pltpu.VMEM((text, hd), BF16),
            pltpu.VMEM((total, hd), BF16),
            pltpu.VMEM((2, B, rows, hd), BF16),
            pltpu.SemaphoreType.REGULAR, pltpu.SemaphoreType.REGULAR,
            pltpu.SemaphoreType.REGULAR, pltpu.SemaphoreType.REGULAR,
            sem((5,)), sem((B,)), sem((n,)), sem((heads,)), sem((heads,)),
            sem((slots,)), sem((slots,)), sem((17,)),
        ],
        compiler_params=pltpu.CompilerParams(
            collective_id=0, has_side_effects=True, vmem_limit_bytes=60 * 1024 * 1024
        ),
    )(
        text_len, patch_len, stale_flags.T,
        hidden_in.reshape(rows, width), w, norm_gain, qk_gain[0], text_states[0],
        stale_kv[0].reshape(2, rows, width),
    )
    hid, cache = pl.pallas_call(
        store,
        out_shape=(
            jax.ShapeDtypeStruct(hid.shape, BF16),
            jax.ShapeDtypeStruct(cache.shape, BF16),
        ),
        in_specs=[pl.BlockSpec(memory_space=pl.ANY)] * 2,
        out_specs=(pl.BlockSpec(memory_space=pl.ANY),) * 2,
        scratch_shapes=[sem((2,))],
    )(pltpu.with_memory_space_constraint(hid, pltpu.VMEM), pltpu.with_memory_space_constraint(cache, pltpu.VMEM))
    return (
        hid.reshape(1, micro, tok, width),
        cache.reshape(1, 2, micro, tok, width),
    )


def solution(mesh):
    in_specs = (
        P(None, "blk", "head"),
        P("section", "blk", None, "head"),
        P("section", None),
        P("section", None, None),
        P("section", None, None),
        P(),
        P(),
        P(),
        P("section", None, None, "blk", "head"),
    )
    out_specs = (P("section", None, "blk", "head"), P("section", None, None, "blk", "head"))
    return jax.shard_map(shards, mesh=mesh, in_specs=in_specs, out_specs=out_specs, check_vma=False)
```

```python
import functools

import jax
import jax.numpy as jnp
from jax import lax
from jax.experimental import pallas as pl
from jax.experimental.pallas import tpu as pltpu
from jax.sharding import PartitionSpec as P

MESH = pl.DeviceIdType.MESH
F32 = jnp.float32
BF16 = jnp.bfloat16


def rms(values, gain):
    return values * lax.rsqrt(jnp.mean(values * values, axis=-1, keepdims=True) + 1e-06) * gain


def kernel(
    dims,
    text_len_in, patch_len_in, flags_in,
    hid_in, w_in, row_gain_in, head_gain_in, text_hbm, stale_in,
    hid_out, cache_out,
    text_len, patch_len, flags, row_gain, head_gain,
    X, X1, RES, XN, text_in, TN, W, R, PROJ, ST, TK, TV,
    hid_own, cache_own,
    all_in, clear, both, taken, ls, xr, zs, zr, yr, rr, fs, one,
):
    S, B, heads, hd, micro, tok = dims
    n = B // 2
    slots = (heads + 1) // 2
    rows = micro * tok
    total = B * rows
    width = heads * hd
    depth = w_in.shape[1]
    s, b, h = lax.axis_index("section"), lax.axis_index("blk"), lax.axis_index("head")
    first_owner = (B - heads) // 2
    off = first_owner - 1 + 2 * h if B - heads >= 2 else first_owner
    late = lax.rem(s, 2)
    early = late == 0
    pair = s + 1 - 2 * late
    mate = b + 1 - 2 * lax.rem(b, 2)
    my_half = b // n
    across = lax.rem(b + n, B)
    inner = lax.rem(b, n) // (n // 2) != my_half
    outer = jnp.logical_not(inner)
    j_own = b - off
    owner = (b >= off) & (b < off + heads)
    core = (s, b, 1 - h)
    half = pl.ds(pl.multiple_of(h * width, hd), width)
    other_half = pl.ds(pl.multiple_of((1 - h) * width, hd), width)
    (
        w_send, w_recv, st_send, st_recv, x_send, xm_send, xc_send, xc_recv, x_own, text_recv,
        ym_send, core_send, core_recv, hid_send, hid_recv, cache_send, cache_recv,
    ) = [one.at[i] for i in range(17)]

    def ahead(k):
        return lax.rem(b + k, B)

    def in_half(k):
        return my_half * n + lax.rem(b - my_half * n + k, n)

    def nearest(k):
        return in_half(k) if k < n else k + my_half * (2 * n - 2 - 2 * k) + lax.rem(b, 2)

    def owns(c):
        return (c >= off) & (c < off + heads)

    def near(c):
        return (c // n == my_half) | (c == across)

    def far(c):
        return jnp.logical_not(near(c))

    def remote(src, dst, send, recv, dev):
        return pltpu.make_async_remote_copy(
            src_ref=src, dst_ref=dst, send_sem=send, recv_sem=recv, device_id=dev, device_id_type=MESH
        )

    def arrived(dst, sem):
        pltpu.make_async_copy(dst, dst, sem).wait()

    def sent(src, sem):
        remote(src, src, sem, sem, core).wait_send()

    def push(src, dst, send, recv, target):
        @pl.when(target == b)
        def _():
            pltpu.make_async_copy(src, dst, recv).start()

        @pl.when(target != b)
        def _():
            remote(src, dst, send, recv, (s, target, h)).start()

    def cols_of(j):
        return pl.ds(pl.multiple_of(j * hd, hd), hd)

    def w_cols(j):
        return w_in.at[:, :, cols_of(j)]

    def w_rows(c):
        return W.at[:, pl.ds(pl.multiple_of(c * depth, depth), depth), :]

    def row_block(c):
        return X.at[c, :, half]

    barrier = pltpu.get_barrier_semaphore()

    def hello(*dev):
        pl.semaphore_signal(barrier, inc=1, device_id=dev, device_id_type=MESH)

    for k in range(n):
        hello(pair, in_half(k), h)
    for k in range(1, n):
        hello(s, in_half(k), h)
    hello(*core)
    hello(pair, across, h)
    hello(s, across, h)
    beside = jnp.where(late == 1, s + 1, s - 1)
    linked = (beside >= 0) & (beside < S)
    if S > 2:
        @pl.when(linked)
        def _():
            for k in range(0, B, 2):
                hello(beside, ahead(k), h)

    text_copy = pltpu.make_async_copy(text_hbm, text_in, text_recv)
    text_copy.start()
    small = (
        (text_len_in, text_len), (patch_len_in, patch_len), (flags_in, flags),
        (row_gain_in, row_gain), (head_gain_in, head_gain),
    )
    loads = [pltpu.make_async_copy(src, dst, ls.at[i]) for i, (src, dst) in enumerate(small)]
    for load in loads:
        load.start()

    @pl.when(s == 0)
    def _():
        pltpu.make_async_copy(hid_in, row_block(b), x_own).start()


    with jax.named_scope("barrier"):
        pl.semaphore_wait(barrier, 2 * n + 2 + (linked.astype(jnp.int32) * n if S > 2 else 0))

    pl.semaphore_signal(all_in, inc=1, device_id=(s, across, h), device_id_type=MESH)

    def other_side(c, t, role):
        return 2 * t + lax.rem(c + off + 1 + role, 2)

    def crosses(c, j):
        return (j < heads) & ((j + off) // n != c // n)

    def detours(c, j, role):
        return crosses(c, j) & (lax.rem(j + off + c + role, 2) == 1)

    def send_relayed():
        for t in range(slots):
            j = other_side(b, t, late)

            @pl.when(detours(b, j, late))
            def _():
                remote(w_cols(j), R.at[t], w_send, rr.at[t], (pair, jnp.where(late == 1, b, mate), h)).start()

    def send_crossing(which):
        for k in range(heads):
            j = lax.rem(b + k, heads)

            @pl.when(crosses(b, j) & jnp.logical_not(detours(b, j, late)) & which(j + off))
            def _():
                remote(w_cols(j), w_rows(b), w_send, w_recv, (s, j + off, h)).start()

    def send_staying():
        for k in range(heads):
            j = lax.rem(b + k, heads)

            @pl.when((j + off) // n == my_half)
            def _():
                push(w_cols(j), w_rows(b), w_send, w_recv, j + off)

    def send_stale(which):
        for k in range(heads):
            j = lax.rem(b + k, heads)

            @pl.when(which(j + off))
            def _():
                push(stale_in.at[:, :, cols_of(j)], ST.at[:, b], st_send, st_recv, j + off)

    def relayed(t):
        cb = jnp.where(late == 1, mate, b)
        j = other_side(cb, t, 1 - late)
        return detours(cb, j, 1 - late), remote(R.at[t], w_rows(cb), fs.at[t], w_recv, (pair, j + off, h))

    def relay():
        for t in range(slots):
            used, onward = relayed(t)

            @pl.when(used)
            def _():
                arrived(R.at[t], rr.at[t])
                onward.start()

    def relay_done():
        for t in range(slots):
            used, _ = relayed(t)

            @pl.when(used)
            def _():
                sent(R.at[t], fs.at[t])

    def send_states(which):
        for k in range(2, B, 2):
            @pl.when(which(nearest(k)))
            def _():
                remote(hid_in, row_block(b), x_send, xr.at[b], (s - 1, nearest(k), h)).start()

    def block_to_core(c):
        return remote(row_block(c), row_block(c), xc_send, xc_recv, core)

    @pl.when(s == 1)
    def _():
        send_states(near)

    @pl.when(early)
    def _():
        send_relayed()

        @pl.when(s == 0)
        def _():
            pltpu.make_async_copy(hid_in, row_block(b), x_own).wait()
            remote(row_block(b), row_block(b), xm_send, xr.at[b], (s, mate, h)).start()
            block_to_core(b).start()

        send_stale(near)

        @pl.when(inner)
        def _():
            send_crossing(near)

    def norm_text():
        for load in loads:
            load.wait()
        text_copy.wait()
        TN[...] = rms(text_in[...].astype(F32), row_gain[...]).astype(BF16)

    @pl.when(early)
    def _():
        norm_text()

    with jax.named_scope("all_in"):
        pl.semaphore_wait(all_in, 1)

    @pl.when(early)
    def _():
        send_stale(far)

        @pl.when(outer)
        def _():
            send_crossing(near)

        send_crossing(far)

        @pl.when(s == 0)
        def _():
            with jax.named_scope("xcol"):
                for k in range(2, B, 2):
                    c = nearest(k)
                    arrived(row_block(c), xr.at[c])
                    remote(row_block(c), row_block(c), xm_send, xr.at[c], (s, mate, h)).start()
                    block_to_core(c).start()

        send_staying()

    @pl.when(late == 1)
    def _():
        @pl.when(s == 1)
        def _():
            send_states(far)

        send_relayed()
        norm_text()
        with jax.named_scope("relay"):
            relay()
        send_staying()
        with jax.named_scope("relay_done"):
            relay_done()
        for k in range(2, n, 2):
            pl.semaphore_signal(clear, inc=1, device_id=(s, in_half(k), h), device_id_type=MESH)
        with jax.named_scope("clear"):
            pl.semaphore_wait(clear, n // 2 - 1)
        pl.semaphore_signal(both, inc=1, device_id=core, device_id_type=MESH)
        with jax.named_scope("both"):
            pl.semaphore_wait(both, 1)
        send_crossing(far)
        send_crossing(near)
        send_stale(near)
        send_stale(far)

    def norm_states(values):
        XN[...] = rms(values.astype(F32), row_gain[...]).astype(BF16)

    @pl.when(s == 0)
    def _():
        with jax.named_scope("waitX"):
            for k in range(0, B, 2):
                c = nearest(k) + mate - b
                arrived(row_block(c), xr.at[c])
                block_to_core(c).start()
        with jax.named_scope("waitswap"):
            arrived(X.at[:, :, other_half], xc_recv)

        @pl.when(owner)
        def _():
            norm_states(X[...].reshape(total, 2 * width))
            RES[...] = X[:, :, pl.ds(pl.multiple_of(h * width + j_own * hd, hd), hd)]

    @pl.when(early & jnp.logical_not(owner))
    def _():
        with jax.named_scope("relayW1"):
            relay()

    def text_part():
        @pl.when(owner)
        def _():
            with jax.named_scope("waitW"):
                arrived(W, w_recv)
            text_kv = jnp.dot(
                TN[...], jnp.concatenate([W[1], W[2]], axis=1), preferred_element_type=F32
            ).astype(BF16)
            TK[...] = rms(text_kv[:, :hd].astype(F32), head_gain[1:2, :]).astype(BF16)
            TV[...] = text_kv[:, hd:]

    @pl.when(s == 0)
    def _():
        text_part()

    def col_block(j):
        return X1.at[h, j]

    def to_core(c):
        return remote(col_block(c - off), col_block(c - off), core_send, core_recv, core)

    @pl.when(s > 0)
    def _():
        with jax.named_scope("waitX1"):
            for k in range(0, B, 2):
                c = nearest(k)

                @pl.when(owns(c))
                def _():
                    block = col_block(c - off)
                    arrived(block, zr.at[c - off])
                    remote(block, block, ym_send, yr.at[c - off], (s, mate, h)).start()
                    to_core(c).start()

        pl.semaphore_signal(taken, inc=1, device_id=(s - 1, b, h), device_id_type=MESH)
        with jax.named_scope("waitX1m"):
            for k in range(0, B, 2):
                c = nearest(k) + mate - b

                @pl.when(owns(c))
                def _():
                    arrived(col_block(c - off), yr.at[c - off])
                    to_core(c).start()

        text_part()
        with jax.named_scope("waitX1c"):
            arrived(X1.at[1 - h], core_recv)

        @pl.when(owner)
        def _():
            norm_states(jnp.concatenate([X1[i, j] for i in range(2) for j in range(heads)], axis=1))
            RES[...] = X1[h, j_own].reshape(RES.shape)

    @pl.when(owner)
    def _():
        PROJ[...] = jnp.dot(
            XN[...], jnp.concatenate([W[0], W[1], W[2]], axis=1), preferred_element_type=F32
        )

    def push_cache():
        for t in range(B):
            push(cache_own.at[:, t], cache_out.at[:, :, cols_of(j_own)], cache_send, cache_recv, t)

    def push_hidden():
        for t in range(B):
            push(
                hid_own.at[pl.ds(t * rows, rows), :],
                hid_out.at[:, cols_of(j_own)], hid_send, hid_recv, t,
            )

    @pl.when(owner)
    def _():
        fresh_k = PROJ[:, hd : 2 * hd].astype(BF16)
        fresh_v = PROJ[:, 2 * hd :].astype(BF16)
        cache_own[0] = fresh_k.reshape(B, rows, hd)
        cache_own[1] = fresh_v.reshape(B, rows, hd)
        @pl.when(s == S - 1)
        def _():
            push_cache()

        with jax.named_scope("waitST"):
            arrived(ST, st_recv)
        tok_bits = tok.bit_length() - 1

        def place(shape, axis):
            at = lax.broadcasted_iota(jnp.int32, shape, axis)
            which = lax.shift_right_logical(at, tok_bits) & (micro - 1)
            spot = lax.shift_right_logical(at, rows.bit_length() - 1) * tok + (at & (tok - 1))
            return which, spot

        def per_micro(which, read):
            out = jnp.zeros(which.shape, jnp.int32)
            for m in range(micro):
                out = jnp.where(which == m, read(m), out)
            return out

        which, _ = place((total, hd), 0)
        use_stale = per_micro(which, lambda m: flags[s, m]) == 1
        kept_k = jnp.where(use_stale, ST[0].reshape(total, hd).astype(F32), fresh_k.astype(F32))
        kept_v = jnp.where(use_stale, ST[1].reshape(total, hd).astype(F32), fresh_v.astype(F32))
        keys = rms(kept_k, head_gain[1:2, :]).astype(BF16)
        queries = rms(PROJ[:, :hd], head_gain[0:1, :]).astype(BF16)
        scale = hd**-0.5
        nt = (((1,), (1,)), ((), ()))

        def attend(key_rows, value_rows, mask):
            scores = lax.dot_general(queries, key_rows, nt, preferred_element_type=F32) * scale
            probs = jnp.where(mask, jnp.exp(scores), 0.0)
            num = jnp.dot(probs.astype(BF16), value_rows, preferred_element_type=F32)
            return num, jnp.sum(probs, axis=1, keepdims=True)

        shape = (total, total)
        q_which, _ = place(shape, 0)
        k_which, k_spot = place(shape, 1)
        mask = (q_which == k_which) & (k_spot < per_micro(k_which, lambda m: patch_len[m]))
        num, den = attend(keys, kept_v.astype(BF16), mask)
        text_at = lax.broadcasted_iota(jnp.int32, (total, TK.shape[0]), 1)
        text_num, text_den = attend(TK[...], TV[...], text_at < text_len[0])
        attended = (num + text_num) / (den + text_den)
        hid_own[...] = (RES[...].reshape(total, hd).astype(F32) + attended).astype(BF16)

        @pl.when(s < S - 1)
        def _():
            for k in range(0, B, 2):
                remote(hid_own, col_block(j_own), zs.at[k // 2], zr.at[j_own], (s + 1, ahead(k), h)).start()

        @pl.when(early)
        def _():
            relay()

        @pl.when(s == S - 1)
        def _():
            push_hidden()

    @pl.when(s < S - 1)
    def _():
        with jax.named_scope("taken"):
            pl.semaphore_wait(taken, 1)

        @pl.when(owner)
        def _():
            for k in range(0, B, 2):
                sent(hid_own, zs.at[k // 2])
            push_hidden()
            push_cache()

    with jax.named_scope("waitOut"):
        arrived(hid_out, hid_recv)
        arrived(cache_out, cache_recv)

    @pl.when(owner)
    def _():
        sent(hid_own.at[pl.ds(0, total - rows), :], hid_send)
        sent(cache_own.at[:, pl.ds(0, B - 1)], cache_send)
        sent(w_in.at[:, :, pl.ds(0, width - hd)], w_send)
        sent(stale_in.at[:, :, pl.ds(0, width - hd)], st_send)

    @pl.when(jnp.logical_not(owner))
    def _():
        sent(w_in, w_send)
        sent(stale_in, st_send)

    @pl.when(early)
    def _():
        relay_done()

    @pl.when(s == 0)
    def _():
        sent(X.at[pl.ds(0, n), :, half], xm_send)
        sent(X.at[:, :, half], xc_send)

    @pl.when(s == 1)
    def _():
        sent(X.at[pl.ds(0, n - 1), :, half], x_send)

    @pl.when(s > 0)
    def _():
        sent(X1.at[h, pl.ds(0, heads // 2)], ym_send)
        sent(X1.at[h], core_send)


def store(hid, cache, hid_out, cache_out, done):
    copies = (
        pltpu.make_async_copy(hid, hid_out, done.at[0]),
        pltpu.make_async_copy(cache, cache_out, done.at[1]),
    )
    for copy in copies:
        copy.start()
    for copy in copies:
        copy.wait()


def shards(
    hidden_in, w_qkv, norm_gain, qk_gain, text_states, text_len, patch_len, stale_flags, stale_kv
):
    S, B = lax.axis_size("section"), lax.axis_size("blk")
    micro, tok, width = hidden_in.shape
    hd = qk_gain.shape[2]
    heads = width // hd
    rows = micro * tok
    total = B * rows
    depth = w_qkv.shape[1]
    text = text_states.shape[1]
    n, slots = B // 2, (heads + 1) // 2
    w = w_qkv[0].transpose(1, 0, 2)
    hbm = pl.BlockSpec(memory_space=pltpu.HBM)
    sem = pltpu.SemaphoreType.DMA
    hid, cache = pl.pallas_call(
        functools.partial(kernel, (S, B, heads, hd, micro, tok)),
        out_shape=(
            pltpu.VMEM((rows, width), BF16),
            pltpu.VMEM((2, rows, width), BF16),
        ),
        in_specs=[hbm] * 9,
        out_specs=(pl.BlockSpec(memory_space=pl.ANY),) * 2,
        scratch_shapes=[
            pltpu.SMEM(text_len.shape, jnp.int32),
            pltpu.SMEM(patch_len.shape, jnp.int32),
            pltpu.SMEM(stale_flags.shape[::-1], jnp.int32),
            pltpu.VMEM(norm_gain.shape, F32),
            pltpu.VMEM(qk_gain.shape[1:], F32),
            pltpu.VMEM((B, rows, 2 * width), BF16),
            pltpu.VMEM((2, heads, total, hd), BF16),
            pltpu.VMEM((B, rows, hd), BF16),
            pltpu.VMEM((total, 2 * width), BF16),
            pltpu.VMEM((text, 2 * width), BF16),
            pltpu.VMEM((text, 2 * width), BF16),
            pltpu.VMEM((3, B * depth, hd), BF16),
            pltpu.VMEM((slots, 3, depth, hd), BF16),
            pltpu.VMEM((total, 3 * hd), F32),
            pltpu.VMEM((2, B, rows, hd), BF16),
            pltpu.VMEM((text, hd), BF16),
            pltpu.VMEM((text, hd), BF16),
            pltpu.VMEM((total, hd), BF16),
            pltpu.VMEM((2, B, rows, hd), BF16),
            pltpu.SemaphoreType.REGULAR, pltpu.SemaphoreType.REGULAR,
            pltpu.SemaphoreType.REGULAR, pltpu.SemaphoreType.REGULAR,
            sem((5,)), sem((B,)), sem((n,)), sem((heads,)), sem((heads,)),
            sem((slots,)), sem((slots,)), sem((17,)),
        ],
        compiler_params=pltpu.CompilerParams(
            collective_id=0, has_side_effects=True, vmem_limit_bytes=60 * 1024 * 1024
        ),
    )(
        text_len, patch_len, stale_flags.T,
        hidden_in.reshape(rows, width), w, norm_gain, qk_gain[0], text_states[0],
        stale_kv[0].reshape(2, rows, width),
    )
    hid, cache = pl.pallas_call(
        store,
        out_shape=(
            jax.ShapeDtypeStruct(hid.shape, BF16),
            jax.ShapeDtypeStruct(cache.shape, BF16),
        ),
        in_specs=[pl.BlockSpec(memory_space=pl.ANY)] * 2,
        out_specs=(pl.BlockSpec(memory_space=pl.ANY),) * 2,
        scratch_shapes=[sem((2,))],
    )(pltpu.with_memory_space_constraint(hid, pltpu.VMEM), pltpu.with_memory_space_constraint(cache, pltpu.VMEM))
    return (
        hid.reshape(1, micro, tok, width),
        cache.reshape(1, 2, micro, tok, width),
    )


def solution(mesh):
    in_specs = (
        P(None, "blk", "head"),
        P("section", "blk", None, "head"),
        P("section", None),
        P("section", None, None),
        P("section", None, None),
        P(),
        P(),
        P(),
        P("section", None, None, "blk", "head"),
    )
    out_specs = (P("section", None, "blk", "head"), P("section", None, None, "blk", "head"))
    return jax.shard_map(shards, mesh=mesh, in_specs=in_specs, out_specs=out_specs, check_vma=False)
```
